32 devices in a mesh: wave: 8 (over y, x, core), lev: 4 (over z).
Axes of the slice: x: 2, y: 2, z: 4, core: 2. Of those that a mesh axis runs over, the one named last changes fastest.
Arguments:
- spec: bfloat16 [16, 128, 640], P('wave', 'lev'), may hold values from -1.5 to 1.5
- legendre: bfloat16 [16, 1280, 640], P('wave'), may hold values from -0.25 to 0.25
- layer_depth_share: float32 [16], P('lev'), may hold values from 0.5 to 2
- quad_weight: float32 [1280], replicated, may hold values from 8 to 32
- wave_of_slot: int32 [16], P('wave'), may hold values from 0 to 639, as said below
Outputs:
- tendency: bfloat16 [16, 128, 640], P('wave', 'lev')
The draws below stay inside these ranges and needn't reach their ends.
Inputs may be any that keep to these rules, and one draw needn't show every extreme that they name: `wave_of_slot`: slots 2 i and 2 i + 1 hold wavenumbers m and 639 - m; no wavenumber appears twice.
All inputs are finite; a program needn't handle non-finite values.
Results may differ from the reference program's by a relative error of at most 0.0047.
The reference program's roundings to bfloat16 on the way count: a program that leaves them out, or rounds other values in their place, can miss the bound.
Values may be sent and summed in bfloat16 or wider, within the bound.
No kernel may reach another device: no remote copies, remote signals or barrier semaphores. Data moves between devices by JAX's collectives and lax.ppermute only.
A program may use at most 128 MiB of HBM per device.

```python
import math
import jax
import jax.numpy as jnp
from jax import lax

LAT = 1280
ORDER_SPAN = 640
QUANTITY_TOTAL = 4
EASTWARD_MODES = 16
LEVELS = 16
COLS = 128
MAXLON = 2576
N_LEV = 4


def draw_wave_of_slot(key, part):
    chosen = jax.random.permutation(key, ORDER_SPAN // 2)[:EASTWARD_MODES // 2].astype(jnp.int32)
    return jnp.stack([chosen, ORDER_SPAN - 1 - chosen], axis=1).reshape(EASTWARD_MODES)


def level_of(own_key, shape, cuts, smallest, high):
    gain, own = 1.0, jax.random.fold_in(own_key, 6)
    for dim, parts in cuts:
        draws = jnp.exp(jax.random.uniform(jax.random.fold_in(own, dim), (parts,), jnp.float32, smallest / len(cuts), high / len(cuts)))
        gain = gain * jnp.repeat(draws, shape[dim] // parts).reshape([-1 if axis == dim else 1 for axis in range(len(shape))])
    return gain


def noise(key, shape, scale, reach, pieces=(), kind=jnp.bfloat16):
    level = level_of(key, shape, pieces, -0.22, 0.18) if pieces else 1.0
    values = jax.random.normal(key, shape, jnp.float32) * scale * level
    return jnp.minimum(jnp.maximum(values, -reach), reach).astype(kind)


def setup_inputs(seed: int = 0) -> dict:
    key_of = jax.random.split(jax.random.key(seed), 6)
    spec = noise(key_of[0], (EASTWARD_MODES, COLS, ORDER_SPAN), EASTWARD_MODES ** -0.5, 1.5, ((0, 8), (1, 4)))
    legendre = noise(key_of[1], (EASTWARD_MODES, LAT, ORDER_SPAN), ORDER_SPAN ** -0.5, 0.25, ((0, 8),))
    layer_depth_share = jnp.clip(jnp.exp(math.log(2.0) - 1.3862944 * jax.random.uniform(key_of[2], (LEVELS,), jnp.float32) ** level_of(key_of[2], (LEVELS,), ((0, 4),), -0.2, 0.2)), 0.5, 2.0)
    quad_weight = jnp.clip(jnp.exp(jax.random.uniform(key_of[3], (LAT,), jnp.float32, math.log(8.0), math.log(32.0))), 8.0, 32.0)
    wave_of_slot = draw_wave_of_slot(jax.random.fold_in(key_of[5], 71), 0)
    return {"spec": spec, "legendre": legendre, "layer_depth_share": layer_depth_share, "quad_weight": quad_weight, "wave_of_slot": wave_of_slot}


full_turn = 2.0 * math.pi


def rate_bundle(eastward_velocity, northward_velocity, local_curl_spin, thermal_state, planetary_rotation_effect, processor_dimension):
    absolute = local_curl_spin + planetary_rotation_effect
    return jnp.stack([absolute * eastward_velocity, absolute * northward_velocity,
                      0.5 * (eastward_velocity * eastward_velocity + northward_velocity * northward_velocity),
                      eastward_velocity * thermal_state], axis=processor_dimension)


def reference(spec, legendre, layer_depth_share, quad_weight, wave_of_slot):
    layers_on_processor = LEVELS // N_LEV
    degree_index = jnp.arange(ORDER_SPAN, dtype=jnp.int32)
    valid_cols = degree_index[None, :] < (ORDER_SPAN - wave_of_slot)[:, None]
    screened_entries = jnp.where(valid_cols[:, None, :], spec, jnp.zeros_like(spec))

    def inverse_one(inputs):
        leg_table, coeffs = inputs
        return jnp.dot(leg_table, coeffs.T, preferred_element_type=jnp.float32).astype(jnp.bfloat16)

    fourier = jnp.moveaxis(lax.map(inverse_one, (legendre, screened_entries)), 1, 0)
    points = jnp.arange(MAXLON, dtype=jnp.int32)
    weight_two = jnp.where(wave_of_slot == 0, 1.0, 2.0).astype(jnp.float32)

    def grid_one(inputs):
        latitude, coeffs = inputs
        length = 20 + 4 * jnp.minimum(latitude, LAT - 1 - latitude)
        length_f = length.astype(jnp.float32)
        phase_int = (wave_of_slot[:, None] * points[None, :]) % length
        angles = phase_int.astype(jnp.float32) * full_turn / length_f
        cosine = jnp.cos(angles)
        sine_vals = jnp.sin(angles)
        resolved = 2 * wave_of_slot < length
        amplitude = jnp.where(resolved, weight_two, 0.0)[:, None]
        split_parts = coeffs.reshape(EASTWARD_MODES, N_LEV, 2, QUANTITY_TOTAL, layers_on_processor)
        real_part = split_parts[:, :, 0].reshape(EASTWARD_MODES, -1)
        imag_part = split_parts[:, :, 1].reshape(EASTWARD_MODES, -1)
        grid_vals = jnp.dot(real_part.T, (amplitude * cosine).astype(jnp.bfloat16), preferred_element_type=jnp.float32)
        grid_vals = grid_vals - jnp.dot(imag_part.T, (amplitude * sine_vals).astype(jnp.bfloat16), preferred_element_type=jnp.float32)
        grid_vals = grid_vals.reshape(N_LEV, QUANTITY_TOTAL, layers_on_processor, MAXLON)
        planetary_rotation_effect = 2.0 * jnp.cos((latitude.astype(jnp.float32) + 0.5) * (math.pi / LAT))
        products = rate_bundle(grid_vals[:, 0], grid_vals[:, 1], grid_vals[:, 2], grid_vals[:, 3], planetary_rotation_effect, 1)
        products = products.astype(jnp.bfloat16).reshape(N_LEV * QUANTITY_TOTAL * layers_on_processor, MAXLON)
        live_mask = (points[None, :] < length) & resolved[:, None]
        cos_back = jnp.where(live_mask, cosine, 0.0).astype(jnp.bfloat16)
        sin_back = jnp.where(live_mask, sine_vals, 0.0).astype(jnp.bfloat16)
        row_scale = quad_weight[latitude] / length_f
        real_back = jnp.dot(products, cos_back.T, preferred_element_type=jnp.float32) * row_scale
        imag_back = -jnp.dot(products, sin_back.T, preferred_element_type=jnp.float32) * row_scale
        merged = jnp.stack([real_back.T.reshape(EASTWARD_MODES, N_LEV, QUANTITY_TOTAL, layers_on_processor),
                            imag_back.T.reshape(EASTWARD_MODES, N_LEV, QUANTITY_TOTAL, layers_on_processor)], axis=2)
        return merged.reshape(EASTWARD_MODES, COLS).astype(jnp.bfloat16)

    tend_rows = lax.map(grid_one, (jnp.arange(LAT, dtype=jnp.int32), fourier))

    def direct_one(inputs):
        leg_table, coeffs = inputs
        return jnp.dot(coeffs.T, leg_table, preferred_element_type=jnp.float32)

    tendency = lax.map(direct_one, (legendre, jnp.moveaxis(tend_rows, 1, 0)))
    thermal_state = screened_entries.reshape(EASTWARD_MODES, N_LEV, 2, QUANTITY_TOTAL, layers_on_processor, ORDER_SPAN)[:, :, :, 3].astype(jnp.float32)
    scaled_entries = thermal_state * layer_depth_share.reshape(N_LEV, 1, layers_on_processor, 1)
    scaled_entries = jnp.moveaxis(scaled_entries, 2, 1).reshape(EASTWARD_MODES, 2, LEVELS, ORDER_SPAN)
    below_sum = jnp.flip(jnp.cumsum(jnp.flip(scaled_entries, 2), 2), 2)
    geopot = jnp.moveaxis(below_sum.reshape(EASTWARD_MODES, 2, N_LEV, layers_on_processor, ORDER_SPAN), 1, 2)
    tendency = tendency.reshape(EASTWARD_MODES, N_LEV, 2, QUANTITY_TOTAL, layers_on_processor, ORDER_SPAN)
    tendency = tendency.at[:, :, :, 2].add(geopot)
    tendency = jnp.where(valid_cols[:, None, None, None, None, :], tendency, 0.0)
    return tendency.reshape(EASTWARD_MODES, COLS, ORDER_SPAN).astype(jnp.bfloat16)
```

```python
import math

import numpy as np
import jax
import jax.numpy as jnp
from jax import lax
from jax.experimental import pallas as pl
from jax.experimental.pallas import tpu as pltpu
from jax.sharding import PartitionSpec as P

bf16 = jnp.bfloat16
f32 = jnp.float32
FIELDS = 4
IMAGES = 4
LANES = 128
ROUNDER = 12582912.0
CHUNK = 256
GROUP = 4


def nt(a, b):
    return lax.dot_general(a, b, (((1,), (1,)), ((), ())), preferred_element_type=f32)


def nn(a, b):
    return lax.dot_general(a, b, (((1,), (0,)), ((), ())), preferred_element_type=f32)


def circle_polynomials():
    f = np.cos(np.pi * (np.arange(4000) + 0.5) / 8000) * 0.5
    z = f * f
    out = []
    for values, degree in ((np.cos(2 * np.pi * f), 6), (np.sin(2 * np.pi * f) / f, 6)):
        fit = np.polynomial.chebyshev.Chebyshev.fit(z, values, degree, domain=[0, 0.25])
        out.append([float(c) for c in fit.convert(kind=np.polynomial.Polynomial).coef])
    return out


COS_POLY, SIN_POLY = circle_polynomials()


def horner(z, coefs):
    acc = jnp.full_like(z, coefs[-1])
    for c in coefs[-2::-1]:
        acc = acc * z + c
    return acc


def cos_sin(count, length, inverse):
    turns = (count * inverse + ROUNDER) - ROUNDER
    f = (count - turns * length) * inverse
    z = f * f
    return horner(z, COS_POLY), f * horner(z, SIN_POLY)


def image_signs():
    return np.array([[1, 1, 1, 1], [-1, 1, -1, 1], [1, 1, -1, -1], [-1, 1, 1, -1]], np.float32)


class Sizes:
    def __init__(self, n_wave, n_lev, slots, cols, lats, span, layers):
        self.n_wave, self.n_lev, self.slots, self.cols = n_wave, n_lev, slots, cols
        self.lats, self.span, self.layers = lats, span, layers
        self.rows = lats // n_wave // 2
        self.half = self.rows // 2
        self.circles = lats // 2
        self.points = self.circles + 11
        self.width = -(-self.points // CHUNK) * CHUNK
        self.tiles = self.width // LANES
        self.sent = self.rows + 8
        self.keys = 8 * n_wave

    def fits(self):
        return (
            self.slots == 2
            and self.cols == 32
            and self.layers == 4
            and self.n_wave == 8
            and self.rows % 16 == 0
            and self.half % (2 * GROUP) == 0
            and self.half % 8 == 0
            and self.half * 4 * self.n_wave == self.lats
            and self.span % LANES == 0
            and (self.n_wave * self.rows) % LANES == 0
            and self.tiles <= 8
        )

    def block_starts(self, owner):
        h = self.half
        return (
            (h * owner, self.circles - h * (owner + 1)),
            (self.lats - h * (owner + 1), self.circles + h * owner),
        )


def spread_matrix(n):
    signs = image_signs()
    out = np.zeros((LANES, 4 * LANES), np.float32)
    for p in range(4):
        for hemi in range(2):
            for field in range(FIELDS):
                for layer in range(n.layers):
                    src = p * 32 + hemi * 16 + field * 4 + layer
                    for image in range(IMAGES):
                        out[src, p * LANES + image * 32 + field * 8 + hemi * 4 + layer] = signs[p, image]
    return out


def order_matrix(n):
    out = np.zeros((LANES, LANES), np.float32)
    for parity in range(2):
        for part in range(2):
            for hemi in range(2):
                for field in range(FIELDS):
                    for layer in range(n.layers):
                        row = hemi * 64 + parity * 32 + part * 16 + field * 4 + layer
                        lane = (parity * 2 + part) * 32 + field * 8 + hemi * 4 + layer
                        out[row, lane] = 1.0
    return out


def live_spec(n, spec, wave):
    degree = lax.broadcasted_iota(jnp.int32, (n.cols, n.span), 1)
    live = degree < n.span - wave
    return jnp.where(live, spec.astype(f32), 0.0), live


def layer_sums(n, masked, share_ref):
    row = lax.broadcasted_iota(jnp.int32, (n.cols, n.span), 0)
    layer = row % n.layers
    weight = jnp.where(
        layer < 2,
        jnp.where(layer == 0, share_ref[0], share_ref[1]),
        jnp.where(layer == 2, share_ref[2], share_ref[3]),
    )
    warm = (row // n.layers) % FIELDS == FIELDS - 1
    y = jnp.where(warm, masked * weight, 0.0)
    y = y + pltpu.roll(y, n.cols - 1, 0)
    return y + pltpu.roll(y, n.cols - 2, 0)


def fetch(pairs, sems):
    copies = [pltpu.make_async_copy(src, dst, sems.at[k]) for k, (src, dst) in enumerate(pairs)]
    for copy in copies:
        copy.start()
    return copies


def forward_kernel(n, wave_hbm, share_hbm, spec_hbm, leg_hbm, out_ref, total_hbm, wave_ref, share_ref, spec_ref, leg, total_ref, acc, sems, leg_sems, done_sem):
    small = fetch(((wave_hbm, wave_ref), (share_hbm, share_ref), (spec_hbm, spec_ref)), sems)
    halves = [(s, hemi) for s in range(2) for hemi in range(2)]
    big = fetch(
        [
            (leg_hbm.at[s, pl.ds(hemi * n.circles, n.circles), :], leg.at[s, pl.ds(hemi * n.circles, n.circles), :])
            for s, hemi in halves
        ],
        leg_sems,
    )
    for copy in small:
        copy.wait()
    tables = []
    for s in range(2):
        masked, _ = live_spec(n, spec_ref[s], wave_ref[s])
        sums = layer_sums(n, masked, share_ref)
        for part in range(2):
            total_ref[2 * s + part : 2 * s + part + 1, :] = sums[part * 16 + 12 : part * 16 + 13, :]
        scaled = masked * jnp.where(wave_ref[s] == 0, 1.0, 2.0)
        none = jnp.zeros_like(scaled[:16])
        for hemi in range(2):
            rows = []
            for parity in range(2):
                mine = wave_ref[s] % 2 == parity
                for part in range(2):
                    chunk = jnp.where(mine, scaled[part * 16 : part * 16 + 16], 0.0)
                    rows += [chunk, none] if hemi == 0 else [none, chunk]
            tables.append(jnp.concatenate(rows, 0).astype(bf16))
    totals_out = pltpu.make_async_copy(total_ref, total_hbm, done_sem)
    totals_out.start()
    for k, (s, hemi) in enumerate(halves):
        big[k].wait()
        piece = nt(leg[s, hemi * n.circles : (hemi + 1) * n.circles, :], tables[k])
        acc[hemi] = piece if s == 0 else acc[hemi] + piece
    even = jnp.where(wave_ref[0] % 2 == 0, wave_ref[0], wave_ref[1])
    lane = lax.broadcasted_iota(jnp.int32, (8, LANES), 1)
    tag = jnp.where(lane < LANES // 2, even // 16, even % 16).astype(f32)
    for owner in range(n.n_wave):
        starts = n.block_starts(owner)
        for b in range(2):
            north = acc[0, starts[0][b] : starts[0][b] + n.half, :]
            south = acc[1, starts[1][b] - n.circles : starts[1][b] - n.circles + n.half, :]
            out_ref[owner, b * n.half : (b + 1) * n.half, :] = (north + south).astype(bf16)
        out_ref[owner, n.rows : n.sent, :] = tag.astype(bf16)
    totals_out.wait()


def grid_kernel(n, got_ref, spread_ref, sign_ref, cor_ref, inv_ref, quad_ref, out_ref, spread, table_a, table_b, coef_a, coef_b, ret, rows):
    device = lax.axis_index("wave")
    first_circle = device * n.half
    top = n.span - 1
    for p in range(4):
        spread[p] = nn(got_ref[...], spread_ref[:, p * LANES : (p + 1) * LANES])
    lane = lax.broadcasted_iota(jnp.int32, (8, LANES), 1)
    lane_f = lane.astype(f32)
    north = (lane // 4) % 2 == 0
    raw = got_rows_f32(n, got_ref)
    tag = jnp.where(lane < LANES // 2, raw * 16.0, raw)
    even_m = tag + pltpu.roll(tag, LANES // 2, 1)
    odd_m = float(top) - even_m

    def sizes(i):
        short = first_circle + i
        return short, n.circles - 1 - short

    def build(i, u, table):
        short, long = sizes(i)
        cut = (short + 6).astype(f32)
        len_s = (20 + 4 * short).astype(f32)
        len_l = (20 + 4 * long).astype(f32)
        inv_s = inv_ref[short]
        inv_l = inv_ref[long]

        def places(point):
            own = point < cut
            return own, jnp.where(own, point, point - cut), jnp.where(own, len_s, len_l), jnp.where(own, inv_s, inv_l)

        tile = lax.broadcasted_iota(jnp.int32, (8, LANES), 0)
        _, j, length, inverse = places((tile * LANES + lane).astype(f32))
        top_c, top_s = cos_sin(j * float(top), length, inverse)
        for t in range(n.tiles):
            own, j, length, inverse = places(lane_f + float(t * LANES))
            c, s = cos_sin(even_m * j, length, inverse)
            tc = jnp.broadcast_to(top_c[t : t + 1, :], (8, LANES))
            ts = jnp.broadcast_to(top_s[t : t + 1, :], (8, LANES))
            odd_c = tc * c + ts * s
            odd_s = ts * c - tc * s
            both = jnp.concatenate([c, s, odd_c, odd_s], 0)
            own = jnp.concatenate([own] * 4, 0)
            two = jnp.concatenate([jnp.where(own, both, 0.0), jnp.where(own, 0.0, both)], 0)
            table[u, :, t * LANES : (t + 1) * LANES] = two.astype(bf16)

    def gather(i, u, coef):
        short, long = sizes(i)
        parts = []
        for circle, row_n, row_s in (
            (short, i, n.half - 1 - i),
            (long, n.rows - 1 - i, n.half + i),
        ):
            length = (20 + 4 * circle).astype(f32)
            even_ok = 2.0 * even_m < length
            odd_ok = 2.0 * odd_m < length
            for p in range(4):
                up = spread[p, pl.ds(row_n, 8, stride=n.sent), :]
                down = spread[p, pl.ds(row_s, 8, stride=n.sent), :]
                parts.append(jnp.where(odd_ok if p > 1 else even_ok, jnp.where(north, up, down), 0.0))
        coef[u] = jnp.transpose(jnp.concatenate(parts, 0)).astype(bf16)

    south = lax.broadcasted_iota(jnp.int32, (8, n.width), 0) // 4
    point = lax.broadcasted_iota(jnp.int32, (8, n.width), 1)
    point_row = lax.broadcasted_iota(jnp.int32, (1, n.width), 1)
    signs = [sign_ref[p : p + 1, :] for p in range(4)]
    group = lane // 32
    kinetic = jnp.where((lane // 8) % FIELDS == 2, 0.5, 1.0)

    def transform(i, u, table, coef):
        short, long = sizes(i)
        cut = short + 6
        tab = table[u]
        grid = nn(coef[u], tab).reshape(IMAGES, FIELDS, 8, n.width)
        spin = jnp.where(point < cut, cor_ref[short], cor_ref[long])
        spin = jnp.where(south == 0, spin, -spin)
        x, y, curl, warm = grid[:, 0], grid[:, 1], grid[:, 2], grid[:, 3]
        absolute = curl + spin
        prods = jnp.stack([absolute * x, absolute * y, x * x + y * y, x * warm], 1)
        prods = prods.reshape(LANES, n.width).astype(bf16)
        edge = (point_row == 0) | (point_row == cut - 1) | (point_row == cut) | (point_row == n.points - 1)
        share = jnp.where(edge, 0.5, jnp.where(point_row < n.points, 1.0, 0.0)).astype(bf16)
        total = nt(tab * share, prods)
        for k, circle in enumerate((short, long)):
            length = (20 + 4 * circle).astype(f32)
            even_ok = 2.0 * even_m < length
            odd_ok = 2.0 * odd_m < length
            folded = None
            for p in range(4):
                y = total[(4 * k + p) * 8 : (4 * k + p + 1) * 8] * signs[p]
                y = y + pltpu.roll(y, 64, 1)
                y = y + pltpu.roll(y, 32, 1)
                y = jnp.where(odd_ok if p > 1 else even_ok, y, 0.0)
                folded = y if folded is None else jnp.where(group == p, y, folded)
            weight = jnp.where(north, quad_ref[circle], quad_ref[n.lats - 1 - circle]) * (inv_ref[circle] * kinetic)
            ret[k, i] = folded * weight

    def ready(start, table, coef):
        for u in range(GROUP):
            i = jnp.minimum(start + u, n.half - 1)
            build(i, u, table)
            gather(i, u, coef)

    def work(start, table, coef):
        for u in range(GROUP):
            transform(start + u, u, table, coef)

    def step(k, carry):
        start = 2 * GROUP * k
        ready(start + GROUP, table_b, coef_b)
        work(start, table_a, coef_a)
        ready(start + 2 * GROUP, table_a, coef_a)
        work(start + GROUP, table_b, coef_b)
        return carry

    ready(0, table_a, coef_a)
    lax.fori_loop(0, n.half // (2 * GROUP), step, 0)

    def place(i, carry):
        other = n.half - 1 - i
        rows[pl.ds(i, 8, stride=n.rows), :] = jnp.where(north, ret[0, i], ret[0, other])
        rows[pl.ds(n.half + i, 8, stride=n.rows), :] = jnp.where(north, ret[1, other], ret[1, i])
        return carry

    lax.fori_loop(0, n.half, place, 0, unroll=4)
    out_ref[...] = rows[...].astype(bf16)


def got_rows_f32(n, got_ref):
    pieces = [got_ref[src * n.sent + n.rows : src * n.sent + n.rows + 8, :].astype(f32)[:1] for src in range(n.n_wave)]
    return jnp.concatenate(pieces, 0)


def back_kernel(n, wave_hbm, share_hbm, *refs):
    deeper_hbm = refs[: n.n_lev - 1]
    spec_ref, back_ref, order_ref, leg, out_ref, wave_ref, share_ref, deeper_ref, turn, sems = refs[n.n_lev - 1 :]
    copies = fetch(
        [(wave_hbm, wave_ref), (share_hbm, share_ref)] + [(ref, deeper_ref.at[k]) for k, ref in enumerate(deeper_hbm)],
        sems,
    )
    for owner in range(n.n_wave):
        starts = n.block_starts(owner)
        for b in range(2):
            block = back_ref[owner * n.rows + b * n.half : owner * n.rows + (b + 1) * n.half, :]
            for hemi in range(2):
                at = starts[hemi][b] - hemi * n.circles
                turn[hemi, at : at + n.half, :] = block
    turned = [nt(order_ref[hemi * 64 : hemi * 64 + 64, :], turn[hemi]) for hemi in range(2)]
    row = lax.broadcasted_iota(jnp.int32, (n.cols, n.span), 0)
    target = (row // n.layers) % FIELDS == 2
    for copy in copies:
        copy.wait()
    deeper = None
    for k in range(n.n_lev - 1):
        deeper = deeper_ref[k] if deeper is None else deeper + deeper_ref[k]
    for s in range(2):
        masked, live = live_spec(n, spec_ref[s], wave_ref[s])
        high = pltpu.roll(layer_sums(n, masked, share_ref), n.cols - n.layers, 0)
        if deeper is not None:
            low = jnp.where(row < 16, deeper[2 * s : 2 * s + 1], deeper[2 * s + 1 : 2 * s + 2])
            high = high + low
        even = wave_ref[s] % 2 == 0
        tendency = jnp.where(target, high, 0.0)
        for hemi in range(2):
            mine = jnp.where(even, turned[hemi][:32], turned[hemi][32:])
            tendency = tendency + nn(mine.astype(bf16), leg[s, hemi * n.circles : (hemi + 1) * n.circles, :])
        out_ref[s] = jnp.where(live, tendency, 0.0).astype(bf16)


def smem():
    return pl.BlockSpec(memory_space=pltpu.SMEM)


def vmem():
    return pl.BlockSpec(memory_space=pltpu.VMEM)


def hbm():
    return pl.BlockSpec(memory_space=pltpu.HBM)


def grid_call(n, got, quad_weight):
    params = pltpu.CompilerParams(vmem_limit_bytes=24 * 1024 * 1024)
    all_rows = n.n_wave * n.rows
    circle = np.arange(n.circles)
    spin = (2.0 * np.cos((circle + 0.5) * (math.pi / n.lats))).astype(np.float32)
    inverse = (1.0 / (20 + 4 * circle)).astype(np.float32)
    signs = np.zeros((8, LANES), np.float32)
    signs[:4] = np.repeat(image_signs(), LANES // IMAGES, axis=1)
    return pl.pallas_call(
        lambda *refs: grid_kernel(n, *refs),
        out_shape=jax.ShapeDtypeStruct((all_rows, LANES), bf16),
        in_specs=[vmem(), vmem(), vmem(), smem(), smem(), smem()],
        out_specs=vmem(),
        scratch_shapes=[
            pltpu.VMEM((4, n.n_wave * n.sent, LANES), f32),
            pltpu.VMEM((GROUP, n.keys, n.width), bf16),
            pltpu.VMEM((GROUP, n.keys, n.width), bf16),
            pltpu.VMEM((GROUP, LANES, n.keys), bf16),
            pltpu.VMEM((GROUP, LANES, n.keys), bf16),
            pltpu.VMEM((2, n.half, 8, LANES), f32),
            pltpu.VMEM((all_rows, LANES), f32),
        ],
        compiler_params=params,
        name="grid_stage",
    )(
        got,
        jnp.asarray(spread_matrix(n), bf16),
        jnp.asarray(signs),
        jnp.asarray(spin),
        jnp.asarray(inverse),
        quad_weight,
    )


def fast_body(n, spec, legendre, layer_depth_share, quad_weight, wave_of_slot):
    params = pltpu.CompilerParams(vmem_limit_bytes=24 * 1024 * 1024)
    all_rows = n.n_wave * n.rows
    dma = pltpu.SemaphoreType.DMA
    small = [pltpu.SMEM((2,), jnp.int32), pltpu.SMEM((n.layers,), f32)]
    sent, totals = pl.pallas_call(
        lambda *refs: forward_kernel(n, *refs),
        out_shape=(
            jax.ShapeDtypeStruct((n.n_wave, n.sent, LANES), bf16),
            jax.ShapeDtypeStruct((4, n.span), f32),
        ),
        in_specs=[hbm()] * 4,
        out_specs=(vmem(), hbm()),
        scratch_shapes=small
        + [
            pltpu.VMEM(spec.shape, bf16),
            pltpu.VMEM(legendre.shape, bf16),
            pltpu.VMEM((4, n.span), f32),
            pltpu.VMEM((2, n.circles, LANES), f32),
            dma((3,)),
            dma((4,)),
            dma,
        ],
        compiler_params=params,
        name="legendre_forward",
    )(wave_of_slot, layer_depth_share, spec, legendre)
    deeper = [
        lax.ppermute(totals, "lev", [(i, i - hop) for i in range(hop, n.n_lev)]) for hop in range(1, n.n_lev)
    ]
    got = lax.all_to_all(sent, "wave", split_axis=0, concat_axis=0, tiled=True)
    out = grid_call(n, got.reshape(n.n_wave * n.sent, LANES), quad_weight)
    back = lax.all_to_all(
        out.reshape(n.n_wave, n.rows, LANES), "wave", split_axis=0, concat_axis=0, tiled=True
    )
    return pl.pallas_call(
        lambda *refs: back_kernel(n, *refs),
        out_shape=jax.ShapeDtypeStruct(spec.shape, bf16),
        in_specs=[hbm()] * (n.n_lev + 1) + [vmem()] * 4,
        out_specs=vmem(),
        scratch_shapes=small
        + [
            pltpu.VMEM((max(n.n_lev - 1, 1), 4, n.span), f32),
            pltpu.VMEM((2, n.circles, LANES), bf16),
            dma((n.n_lev + 1,)),
        ],
        compiler_params=params,
        name="legendre_back",
    )(
        wave_of_slot,
        layer_depth_share,
        *deeper,
        spec,
        back.reshape(all_rows, LANES),
        jnp.asarray(order_matrix(n), bf16),
        legendre,
    )


full_turn = 2.0 * math.pi


def carried_in(part, axis, combine, identity):
    count = lax.axis_size(axis)
    place = lax.axis_index(axis)
    ahead = count - 1 - place
    gathered = lax.all_gather(part, axis)
    state = jnp.zeros_like(part) + jnp.asarray(identity, part.dtype)

    def one(hop, state):
        source = count - 1 - hop
        return combine(state, lax.dynamic_index_in_dim(gathered, source, 0, False))

    return lax.fori_loop(0, ahead, one, state)


def rate_bundle(
    eastward_velocity,
    northward_velocity,
    local_curl_spin,
    thermal_state,
    planetary_rotation_effect,
    processor_dimension,
):
    absolute = local_curl_spin + planetary_rotation_effect
    return jnp.stack(
        [
            absolute * eastward_velocity,
            absolute * northward_velocity,
            0.5 * (eastward_velocity * eastward_velocity + northward_velocity * northward_velocity),
            eastward_velocity * thermal_state,
        ],
        axis=processor_dimension,
    )


def row_latitudes(device, per_dev, total_lat):
    row_ids = jnp.arange(per_dev, dtype=jnp.int32)
    quarter = per_dev // 4
    block_ids = row_ids // 4
    hemisphere = row_ids // 2 % 2
    member = row_ids % 2
    first_dist = device * quarter + block_ids
    pole_dist = jnp.where(member == 0, first_dist, total_lat // 2 - 1 - first_dist)
    return jnp.where(hemisphere == 0, pole_dist, total_lat - 1 - pole_dist)


def add_terms(earlier, later):
    return earlier + later


def general_body(spec, legendre, layer_depth_share, quad_weight, wave_of_slot):
    number_of_slots, columns, degree_list = spec.shape
    total_lat = legendre.shape[1]
    groups = lax.axis_size("wave")
    device = lax.axis_index("wave")
    per_dev = total_lat // groups
    layers_on_processor = layer_depth_share.shape[0]
    field_stack = columns // (2 * layers_on_processor)
    flat_rows = field_stack * layers_on_processor
    max_points = 20 + 4 * (total_lat // 2 - 1)
    all_waves = lax.all_gather(wave_of_slot, "wave", axis=0, tiled=True)
    wave_count = all_waves.shape[0]
    weight_two = jnp.where(all_waves == 0, 1.0, 2.0).astype(jnp.float32)
    degree_index = jnp.arange(degree_list, dtype=jnp.int32)
    valid_cols = degree_index[None, :] < (degree_list - wave_of_slot)[:, None]
    screened_entries = jnp.where(valid_cols[:, None, :], spec, jnp.zeros_like(spec))
    thermal_state = screened_entries.reshape(
        number_of_slots, 2, field_stack, layers_on_processor, degree_list
    )[:, :, 3].astype(jnp.float32)
    scaled_entries = thermal_state * layer_depth_share[None, None, :, None]
    below_sum = jnp.flip(jnp.cumsum(jnp.flip(scaled_entries, 2), 2), 2)
    deeper = carried_in(
        below_sum[:, :, 0],
        "lev",
        add_terms,
        jnp.zeros((number_of_slots, 2, degree_list), jnp.float32),
    )
    geopot = below_sum + deeper[:, :, None, :]
    fourier = jnp.einsum(
        "sln,scn->lsc", legendre, screened_entries, preferred_element_type=jnp.float32
    ).astype(jnp.bfloat16)
    send_order = row_latitudes(
        jnp.arange(groups, dtype=jnp.int32)[:, None], per_dev, total_lat
    ).reshape(-1)
    send_rows = jnp.take(fourier, send_order, axis=0).reshape(total_lat, number_of_slots * columns)
    received = lax.all_to_all(send_rows, "wave", split_axis=0, concat_axis=1, tiled=True)
    coeffs = received.reshape(per_dev, wave_count, 2, flat_rows)
    latitudes = row_latitudes(device, per_dev, total_lat)
    lengths = 20 + 4 * jnp.minimum(latitudes, total_lat - 1 - latitudes)
    planetary_rotation_effect = 2.0 * jnp.cos(
        (latitudes.astype(jnp.float32) + 0.5) * (math.pi / total_lat)
    )
    row_scale = quad_weight[latitudes] / lengths.astype(jnp.float32)
    quarter = per_dev // 4
    pair_points = max_points + 20
    tile_count = -(-pair_points // 128)
    padded = tile_count * 128
    pair_len = lengths.reshape(quarter, 2, 2)[:, 0, :]
    first_len = pair_len[:, 0:1]
    second_len = pair_len[:, 1:2]
    points = jnp.arange(padded, dtype=jnp.int32)[None, :]
    first_lat = points < first_len
    in_pair = points < pair_points
    local_idx = jnp.where(first_lat, points, points - first_len)
    point_len = jnp.where(first_lat, first_len, second_len)
    phase_int = all_waves[None, :, None] * local_idx[:, None, :] % point_len[:, None, :]
    angles = phase_int.astype(jnp.float32) * full_turn / point_len.astype(jnp.float32)[:, None, :]
    cosine = jnp.cos(angles)
    sine_vals = jnp.sin(angles)
    resolved = (2 * all_waves[None, :, None] < point_len[:, None, :]) & in_pair[:, None, :]
    amplitude = jnp.where(resolved, weight_two[None, :, None], 0.0)
    forward_tab = jnp.concatenate([amplitude * cosine, -(amplitude * sine_vals)], 1).astype(
        jnp.bfloat16
    )
    back_tab = jnp.concatenate(
        [jnp.where(resolved, cosine, 0.0), -jnp.where(resolved, sine_vals, 0.0)], 1
    ).astype(jnp.bfloat16)
    forward_tiles = forward_tab.reshape(quarter, 2 * wave_count, tile_count, 128)
    back_tiles = back_tab.reshape(quarter, 2 * wave_count, tile_count, 128)
    tile_start = jnp.arange(tile_count, dtype=jnp.int32)[None, :] * 128
    owner_second = tile_start + 128 > first_len
    boundary = first_len[:, 0] // 128
    is_bound = jnp.arange(tile_count, dtype=jnp.int32)[None, :] == boundary[:, None]
    first_tiles = first_lat.reshape(quarter, tile_count, 128)
    stacked = coeffs.reshape(quarter, 2, 2, wave_count, 2, flat_rows).transpose(0, 1, 2, 4, 3, 5)
    stacked = stacked.reshape(quarter, 2, 2, 2 * wave_count, flat_rows)
    coef_tiles = jnp.where(
        owner_second[:, None, :, None, None],
        stacked[:, :, 1][:, :, None],
        stacked[:, :, 0][:, :, None],
    )
    grid_tiles = jnp.einsum(
        "qatkf,qktp->qaftp", coef_tiles, forward_tiles, preferred_element_type=jnp.float32
    )
    bound_fwd = jnp.take_along_axis(forward_tiles, boundary[:, None, None, None], axis=2)[:, :, 0]
    bound_back = jnp.take_along_axis(back_tiles, boundary[:, None, None, None], axis=2)[:, :, 0]
    edge_grid = jnp.einsum(
        "qakf,qkp->qafp", stacked[:, :, 0], bound_fwd, preferred_element_type=jnp.float32
    )
    use_edge = is_bound[:, :, None] & first_tiles
    grid_tiles = jnp.where(use_edge[:, None, None], edge_grid[:, :, :, None, :], grid_tiles)
    grid_vals = grid_tiles.reshape(quarter, 2, field_stack, layers_on_processor, padded)
    row_cor = planetary_rotation_effect.reshape(quarter, 2, 2)
    point_cor = jnp.where(first_lat[:, None, :], row_cor[:, :, 0:1], row_cor[:, :, 1:2])[
        :, :, None, :
    ]
    products = rate_bundle(
        grid_vals[:, :, 0], grid_vals[:, :, 1], grid_vals[:, :, 2], grid_vals[:, :, 3], point_cor, 2
    )
    products = products.astype(jnp.bfloat16).reshape(quarter, 2, flat_rows, tile_count, 128)
    keep = jnp.where(owner_second[:, :, None], jnp.logical_not(first_tiles), first_tiles)
    main_prods = jnp.where(keep[:, None, None], products, jnp.zeros_like(products))
    per_tile = jnp.einsum(
        "qaftp,qktp->qatkf", main_prods, back_tiles, preferred_element_type=jnp.float32
    )
    bound_prods = jnp.take_along_axis(products, boundary[:, None, None, None, None], axis=3)[
        :, :, :, 0
    ]
    bound_first = jnp.take_along_axis(first_tiles, boundary[:, None, None], axis=1)[:, 0]
    bound_prods = jnp.where(bound_first[:, None, None, :], bound_prods, jnp.zeros_like(bound_prods))
    edge_back = jnp.einsum(
        "qafp,qkp->qakf", bound_prods, bound_back, preferred_element_type=jnp.float32
    )
    owner_mask = owner_second[:, None, :, None, None]
    first_ret = jnp.sum(jnp.where(owner_mask, 0.0, per_tile), axis=2) + edge_back
    second_ret = jnp.sum(jnp.where(owner_mask, per_tile, 0.0), axis=2)
    returned = jnp.stack([first_ret, second_ret], axis=2)
    returned = (returned * row_scale.reshape(quarter, 2, 2)[:, :, :, None, None]).astype(
        jnp.bfloat16
    )
    out_rows = returned.reshape(quarter, 2, 2, 2, wave_count, flat_rows).transpose(0, 1, 2, 4, 3, 5)
    out_rows = out_rows.reshape(per_dev, wave_count * columns)
    gathered_rows = lax.all_to_all(out_rows, "wave", split_axis=1, concat_axis=0, tiled=True)
    inverse = (
        jnp.zeros((total_lat,), jnp.int32)
        .at[send_order]
        .set(jnp.arange(total_lat, dtype=jnp.int32))
    )
    back_fourier = jnp.take(gathered_rows, inverse, axis=0).reshape(
        total_lat, number_of_slots, columns
    )
    tendency = jnp.einsum(
        "lsc,sln->scn", back_fourier, legendre, preferred_element_type=jnp.float32
    )
    tendency = tendency.reshape(number_of_slots, 2, field_stack, layers_on_processor, degree_list)
    tendency = tendency.at[:, :, 2].add(geopot)
    tendency = jnp.where(valid_cols[:, None, None, None, :], tendency, 0.0)
    return tendency.reshape(number_of_slots, columns, degree_list).astype(jnp.bfloat16)


def solution(mesh):
    def body(spec, legendre, layer_depth_share, quad_weight, wave_of_slot):
        slots, cols, span = spec.shape
        layers = layer_depth_share.shape[0]
        n = Sizes(mesh.shape["wave"], mesh.shape["lev"], slots, cols, legendre.shape[1], span, layers)
        step = (lambda *args: fast_body(n, *args)) if n.fits() else general_body
        return step(spec, legendre, layer_depth_share, quad_weight, wave_of_slot)

    in_specs = (P("wave", "lev", None), P("wave", None, None), P("lev"), P(), P("wave"))
    out_specs = P("wave", "lev", None)
    return jax.shard_map(body, mesh=mesh, in_specs=in_specs, out_specs=out_specs, check_vma=False)
```

```python
import math

import numpy as np
import jax
import jax.numpy as jnp
from jax import lax
from jax.experimental import pallas as pl
from jax.experimental.pallas import tpu as pltpu
from jax.sharding import PartitionSpec as P

bf16 = jnp.bfloat16
f32 = jnp.float32
FIELDS = 4
IMAGES = 4
LANES = 128
ROUNDER = 12582912.0
CHUNK = 256
GROUP = 10
PIECES = 2
FLIGHT = 2


def nt(a, b):
    return lax.dot_general(a, b, (((1,), (1,)), ((), ())), preferred_element_type=f32)


def nn(a, b):
    return lax.dot_general(a, b, (((1,), (0,)), ((), ())), preferred_element_type=f32)


def circle_polynomials():
    f = np.cos(np.pi * (np.arange(4000) + 0.5) / 8000) * 0.505
    z = f * f
    out = []
    for values in (np.cos(np.pi * f), np.sin(np.pi * f) / f):
        fit = np.polynomial.chebyshev.Chebyshev.fit(z, math.sqrt(2.0) * values, 4, domain=[0, 0.2551])
        out.append([float(c) for c in fit.convert(kind=np.polynomial.Polynomial).coef])
    return out


COS_POLY, SIN_POLY = circle_polynomials()


def horner(z, coefs):
    acc = z * coefs[-1] + coefs[-2]
    for c in coefs[-3::-1]:
        acc = acc * z + c
    return acc


def cos_sin(count, length, inverse):
    turns = (count * inverse + ROUNDER) - ROUNDER
    f = (count - turns * length) * inverse
    z = f * f
    half_sin = f * horner(z, SIN_POLY)
    return 1.0 - half_sin * half_sin, half_sin * horner(z, COS_POLY)


def image_signs():
    return np.array([[1, 1, 1, 1], [-1, 1, -1, 1], [1, 1, -1, -1], [-1, 1, 1, -1]], np.float32)


class Sizes:
    def __init__(self, n_wave, n_lev, slots, cols, lats, span, layers):
        self.n_wave, self.n_lev, self.slots, self.cols = n_wave, n_lev, slots, cols
        self.lats, self.span, self.layers = lats, span, layers
        self.rows = lats // n_wave // 2
        self.half = self.rows // 2
        self.circles = lats // 2
        self.points = self.circles + 11
        self.width = -(-self.points // CHUNK) * CHUNK
        self.tiles = self.width // LANES
        self.sent = self.rows + 8
        self.keys = 8 * n_wave

    def fits(self):
        return (
            self.slots == 2
            and self.cols == 32
            and self.layers == 4
            and self.n_wave == 8
            and self.n_lev == 4
            and self.rows % 16 == 0
            and self.half % (2 * GROUP) == 0
            and self.half % 8 == 0
            and self.half * 4 * self.n_wave == self.lats
            and self.span % LANES == 0
            and (self.n_wave * self.rows) % LANES == 0
            and self.tiles <= 8
        )

    def block_starts(self, owner):
        h = self.half
        return (
            (h * owner, self.circles - h * (owner + 1)),
            (self.lats - h * (owner + 1), self.circles + h * owner),
        )


def order_matrix(n):
    out = np.zeros((LANES, LANES), np.float32)
    for parity in range(2):
        for part in range(2):
            for hemi in range(2):
                for field in range(FIELDS):
                    for layer in range(n.layers):
                        row = hemi * 64 + parity * 32 + part * 16 + field * 4 + layer
                        lane = (parity * 2 + part) * 32 + field * 8 + hemi * 4 + layer
                        out[row, lane] = 1.0
    return out


def live_spec(n, spec, wave):
    degree = lax.broadcasted_iota(jnp.int32, (n.cols, n.span), 1)
    live = degree < n.span - wave
    return jnp.where(live, spec.astype(f32), 0.0), live


def layer_sums(n, masked, share_ref):
    row = lax.broadcasted_iota(jnp.int32, (n.cols, n.span), 0)
    layer = row % n.layers
    weight = jnp.where(
        layer < 2,
        jnp.where(layer == 0, share_ref[0], share_ref[1]),
        jnp.where(layer == 2, share_ref[2], share_ref[3]),
    )
    warm = (row // n.layers) % FIELDS == FIELDS - 1
    y = jnp.where(warm, masked * weight, 0.0)
    y = y + pltpu.roll(y, n.cols - 1, 0)
    return y + pltpu.roll(y, n.cols - 2, 0)


def fetch(pairs, sems):
    copies = [pltpu.make_async_copy(src, dst, sems.at[k]) for k, (src, dst) in enumerate(pairs)]
    for copy in copies:
        copy.start()
    return copies


def forward_kernel(n, wave_hbm, share_hbm, spec_hbm, leg_hbm, out_hbm, total_hbm, leg, high_hbm, wave_ref, share_ref, spec_ref, total_ref, high_ref, acc, sems, leg_sems, done_sems, out_ref, out_sems):
    small = fetch(((wave_hbm, wave_ref), (share_hbm, share_ref), (spec_hbm, spec_ref)), sems)
    size = n.circles // PIECES
    big = [
        [
            pltpu.make_async_copy(leg_hbm.at[s, pl.ds(k * size, size), :], leg.at[s, pl.ds(k * size, size), :], leg_sems.at[s, k])
            for s in range(2)
        ]
        for k in range(2 * PIECES)
    ]
    for pair in big[:FLIGHT]:
        for copy in pair:
            copy.start()
    for copy in small:
        copy.wait()
    row = lax.broadcasted_iota(jnp.int32, (n.cols, n.span), 0)
    target = (row // n.layers) % FIELDS == 2
    tables = [[], []]
    for s in range(2):
        masked, live = live_spec(n, spec_ref[s], wave_ref[s])
        sums = layer_sums(n, masked, share_ref)
        for part in range(2):
            total_ref[2 * s + part : 2 * s + part + 1, :] = sums[part * 16 + 12 : part * 16 + 13, :]
        high_ref[s] = jnp.where(target, pltpu.roll(sums, n.cols - n.layers, 0), 0.0)
        leg[s, n.lats : n.lats + 8, :] = jnp.where(live[:8], 1.0, 0.0).astype(bf16)
        leg[s, n.lats + 8 : n.lats + 16, :] = jnp.full((8, n.span), (1 - wave_ref[s] % 2).astype(f32)).astype(bf16)
        scaled = masked * jnp.where(wave_ref[s] == 0, 1.0, 2.0)
        none = jnp.zeros_like(scaled[:16])
        for hemi in range(2):
            rows = []
            for parity in range(2):
                mine = wave_ref[s] % 2 == parity
                for part in range(2):
                    chunk = jnp.where(mine, scaled[part * 16 : part * 16 + 16], 0.0)
                    rows += [chunk, none] if hemi == 0 else [none, chunk]
            tables[hemi].append(jnp.concatenate(rows, 0).astype(bf16))
    tables = [jnp.concatenate(pair, 1) for pair in tables]
    even = jnp.where(wave_ref[0] % 2 == 0, wave_ref[0], wave_ref[1])
    lane = lax.broadcasted_iota(jnp.int32, (8, LANES), 1)
    tag = jnp.where(lane < LANES // 2, even // 16, even % 16).astype(f32).astype(bf16)
    for owner in range(n.n_wave):
        out_ref[owner, n.rows : n.sent, :] = tag

    def strip(start, count):
        return out_ref.at[:, pl.ds(start, count), :], out_hbm.at[:, pl.ds(start, count), :]

    leaving = fetch(((total_ref, total_hbm), (high_ref, high_hbm), strip(n.rows, 8)), done_sems)
    for k in range(2 * PIECES):
        for copy in big[k]:
            copy.wait()
        if k + FLIGHT < 2 * PIECES:
            for copy in big[k + FLIGHT]:
                copy.start()
        rows = slice(k * size, (k + 1) * size)
        both = jnp.concatenate([leg[0, rows, :], leg[1, rows, :]], 1)
        acc[rows, :] = nt(both, tables[k // PIECES])
        if k >= PIECES and (k + 1) % (PIECES // 2) == 0:
            b = 3 - (k + 1) // (PIECES // 2) + 1
            for owner in range(n.n_wave):
                starts = n.block_starts(owner)
                block = acc[starts[0][b] : starts[0][b] + n.half, :] + acc[starts[1][b] : starts[1][b] + n.half, :]
                out_ref[owner, b * n.half : (b + 1) * n.half, :] = block.astype(bf16)
            copy = pltpu.make_async_copy(*strip(b * n.half, n.half), out_sems.at[b])
            copy.start()
            leaving.append(copy)
    for copy in leaving:
        copy.wait()


def grid_kernel(n, got_ref, sign_ref, near_ref, quad_hbm, total_hbm, out_hbm, pair_hbm, keep_hbm, spread, table_a, table_b, coef_a, coef_b, ret, rows, out, total_ref, pair_ref, keep_ref, quad_ref, out_sem, in_sems, side_sems, inv_ref, cor_ref):
    arriving = fetch(((quad_hbm, quad_ref), (total_hbm, total_ref)), in_sems)
    device = lax.axis_index("wave")
    first_circle = device * n.half
    top = n.span - 1
    lane = lax.broadcasted_iota(jnp.int32, (8, LANES), 1)
    lane_f = lane.astype(f32)
    north = (lane // 4) % 2 == 0
    sent_lane = lax.broadcasted_iota(jnp.int32, (LANES, LANES), 0)
    to = lax.broadcasted_iota(jnp.int32, (LANES, LANES), 1)
    source = (to // 4 % 2) * 16 + (to // 8 % FIELDS) * 4 + to % 4
    for p in range(4):
        pick = jnp.where(sent_lane == source + p * 32, sign_ref[p : p + 1, :], 0.0).astype(bf16)
        wide = nn(got_ref[...], pick)
        for src in range(n.n_wave):
            for r in range(0, n.rows, 8):
                spread[p, pl.ds(r * n.n_wave + src, 8, stride=n.n_wave), :] = wide[src * n.sent + r : src * n.sent + r + 8]
    raw = got_rows_f32(n, got_ref)
    tag = jnp.where(lane < LANES // 2, raw * 16.0, raw)
    even_m = tag + pltpu.roll(tag, LANES // 2, 1)
    odd_m = float(top) - even_m
    even_2 = 2.0 * even_m
    odd_2 = 2.0 * odd_m
    for k in range(2):
        step = lax.broadcasted_iota(jnp.int32, (n.half, LANES), 0)
        circle = first_circle + step if k == 0 else n.circles - 1 - first_circle - step
        inv_ref[k] = 1.0 / (20 + 4 * circle).astype(f32)
        whole = jnp.full((n.half, LANES), 4.0 * n.lats, f32)
        cosine, _ = cos_sin((2 * circle + 1).astype(f32), whole, 1.0 / (4 * n.lats))
        cor_ref[k] = 2.0 * cosine
    tile_point = (lax.broadcasted_iota(jnp.int32, (8, LANES), 0) * LANES + lane).astype(f32)

    def sizes(i):
        short = first_circle + i
        return short, n.circles - 1 - short

    def build(i, u, table):
        short, long = sizes(i)
        cut = (short + 6).astype(f32)
        len_s = (20 + 4 * short).astype(f32)
        len_l = (20 + 4 * long).astype(f32)
        inv_s = inv_ref[0, pl.ds(i, 1), :]
        inv_l = inv_ref[1, pl.ds(i, 1), :]

        def places(point):
            own = point < cut
            return jnp.where(own, point, point - cut), jnp.where(own, len_s, len_l), jnp.where(own, inv_s, inv_l)

        j, length, inverse = places(tile_point)
        top_c, top_s = cos_sin(j * float(top), length, inverse)
        for t in range(n.tiles):
            j, length, inverse = places(lane_f + float(t * LANES))
            c, s = cos_sin(even_m * j, length, inverse)
            tc = jnp.broadcast_to(top_c[t : t + 1, :], (8, LANES))
            ts = jnp.broadcast_to(top_s[t : t + 1, :], (8, LANES))
            span = slice(t * LANES, (t + 1) * LANES)
            table[u, 0:8, span] = c
            table[u, 8:16, span] = s
            table[u, 16:24, span] = tc * c + ts * s
            table[u, 24:32, span] = ts * c - tc * s

    def gather(i, u, coef):
        short, long = sizes(i)
        parts = []
        for circle, row_n, row_s in (
            (short, i, n.half - 1 - i),
            (long, n.rows - 1 - i, n.half + i),
        ):
            length = (20 + 4 * circle).astype(f32)
            for p in range(4):
                up = spread[p, pl.ds(pl.multiple_of(row_n * 8, 8), 8), :]
                down = spread[p, pl.ds(pl.multiple_of(row_s * 8, 8), 8), :]
                seen = (odd_2 if p > 1 else even_2) < length
                parts.append(jnp.where(seen, jnp.where(north, up, down), 0.0))
        coef[u] = jnp.transpose(jnp.concatenate(parts, 0))

    south = lax.broadcasted_iota(jnp.int32, (8, LANES), 0) // 4
    lane_b = lax.broadcasted_iota(jnp.int32, (16, LANES), 1).astype(f32).astype(bf16)
    signs = [sign_ref[p : p + 1, :] for p in range(4)]
    group = lane // 32
    kinetic = jnp.where((lane // 8) % FIELDS == 2, 0.5, 1.0)

    def weights(t, cut):
        edge_at = jnp.clip(cut - t * LANES, -4, LANES + 4).astype(f32) - 0.5
        x = jnp.full((16, LANES), edge_at, f32).astype(bf16) - lane_b
        share = jnp.minimum(jnp.abs(x), 1.0)
        own = jnp.minimum(jnp.maximum(x + 0.5, 0.0), 1.0)
        if t == 0 or (t + 1) * LANES >= n.points:
            point = lax.broadcasted_iota(jnp.int32, (16, LANES), 1) + t * LANES
            ends = (point == 0) | (point == n.points - 1)
            share = share * jnp.where(ends, 0.5, jnp.where(point < n.points, 1.0, 0.0)).astype(bf16)
        own_share = own * share
        return own, 1.0 - own, own_share, share - own_share

    def transform(i, u, table, coef):
        short, long = sizes(i)
        cut = short + 6
        left = coef[u].astype(bf16)
        cor_s = cor_ref[0, pl.ds(i, 1), :]
        cor_l = cor_ref[1, pl.ds(i, 1), :]
        total = None
        for c in range(n.width // CHUNK):
            ahead, behind, spins = [], [], []
            for t in range(c * CHUNK // LANES, (c + 1) * CHUNK // LANES):
                tab = table[u, :, t * LANES : (t + 1) * LANES].astype(bf16)
                own, rest, own_share, rest_share = weights(t, cut)
                ahead.append(jnp.concatenate([tab[:16] * own, tab[16:] * own, tab[:16] * rest, tab[16:] * rest], 0))
                behind.append(
                    jnp.concatenate(
                        [tab[:16] * own_share, tab[16:] * own_share, tab[:16] * rest_share, tab[16:] * rest_share], 0
                    )
                )
                spin = jnp.where(lane < cut - t * LANES, cor_s, cor_l)
                spins.append(jnp.where(south == 0, spin, -spin))
            grid = nn(left, jnp.concatenate(ahead, 1)).reshape(IMAGES, FIELDS, 8, CHUNK)
            x, y, curl, warm = grid[:, 0], grid[:, 1], grid[:, 2], grid[:, 3]
            absolute = curl + jnp.concatenate(spins, 1)
            prods = jnp.stack([absolute * x, absolute * y, x * x + y * y, x * warm], 1)
            piece = nt(jnp.concatenate(behind, 1), prods.reshape(LANES, CHUNK).astype(bf16))
            total = piece if total is None else total + piece
        for k, circle in enumerate((short, long)):
            length = (20 + 4 * circle).astype(f32)
            folded = None
            for p in range(4):
                y = total[(4 * k + p) * 8 : (4 * k + p + 1) * 8] * signs[p]
                y = y + pltpu.roll(y, 64, 1)
                y = y + pltpu.roll(y, 32, 1)
                y = jnp.where((odd_2 if p > 1 else even_2) < length, y, 0.0)
                folded = y if folded is None else jnp.where(group == p, y, folded)
            weight = jnp.where(north, quad_ref[circle], quad_ref[n.lats - 1 - circle])
            ret[k, i] = folded * (weight * (inv_ref[k, pl.ds(i, 1), :] * kinetic))

    def ready(start, table, coef):
        for u in range(GROUP):
            i = jnp.minimum(start + u, n.half - 1)
            build(i, u, table)
            gather(i, u, coef)

    def work(start, table, coef):
        for u in range(GROUP):
            transform(start + u, u, table, coef)

    def step(k, carry):
        start = 2 * GROUP * k
        ready(start + GROUP, table_b, coef_b)
        work(start, table_a, coef_a)
        ready(start + 2 * GROUP, table_a, coef_a)
        work(start + GROUP, table_b, coef_b)
        return carry

    ready(0, table_a, coef_a)
    for copy in arriving:
        copy.wait()
    pair_ref[...] = total_ref[...] + near_ref[...]
    keep_ref[...] = jnp.where(lax.axis_index("lev") % 2 == 0, near_ref[...], 0.0)
    leaving = fetch(((pair_ref, pair_hbm), (keep_ref, keep_hbm)), side_sems)
    lax.fori_loop(0, n.half // (2 * GROUP), step, 0)

    def place(i, carry):
        other = n.half - 1 - i
        rows[pl.ds(i, 8, stride=n.rows), :] = jnp.where(north, ret[0, i], ret[0, other])
        rows[pl.ds(n.half + i, 8, stride=n.rows), :] = jnp.where(north, ret[1, other], ret[1, i])
        return carry

    lax.fori_loop(0, n.half, place, 0, unroll=4)
    out[...] = rows[...].astype(bf16)
    copy = pltpu.make_async_copy(out, out_hbm, out_sem)
    copy.start()
    for side in leaving:
        side.wait()
    copy.wait()


def got_rows_f32(n, got_ref):
    pieces = [got_ref[src * n.sent + n.rows : src * n.sent + n.rows + 8, :].astype(f32)[:1] for src in range(n.n_wave)]
    return jnp.concatenate(pieces, 0)


def back_kernel(n, far_hbm, keep_hbm, high_hbm, back_ref, order_ref, leg, out_ref, turn, far_ref, keep_ref, high_ref, sems):
    arriving = fetch(((far_hbm, far_ref), (keep_hbm, keep_ref), (high_hbm, high_ref)), sems)
    for owner in range(n.n_wave):
        starts = n.block_starts(owner)
        for b in range(2):
            block = back_ref[owner * n.rows + b * n.half : owner * n.rows + (b + 1) * n.half, :]
            for hemi in range(2):
                at = starts[hemi][b] - hemi * n.circles
                turn[hemi, at : at + n.half, :] = block
    turned = [nt(order_ref[hemi * 64 : hemi * 64 + 64, :], turn[hemi]) for hemi in range(2)]
    row = lax.broadcasted_iota(jnp.int32, (n.cols, n.span), 0)
    target = (row // n.layers) % FIELDS == 2
    sums = []
    for s in range(2):
        even = leg[s, n.lats + 8 : n.lats + 16, :].astype(f32)[:1] > 0.5
        for hemi in range(2):
            mine = jnp.where(even, turned[hemi][:32], turned[hemi][32:]).astype(bf16)
            piece = nn(mine, leg[s, hemi * n.circles : (hemi + 1) * n.circles, :])
            sums.append(piece if hemi == 0 else sums.pop() + piece)
    for copy in arriving:
        copy.wait()
    deeper = keep_ref[...] + jnp.where(lax.axis_index("lev") < n.n_lev // 2, far_ref[...], 0.0)
    for s in range(2):
        live = leg[s, n.lats : n.lats + 8, :].astype(f32)[:1] > 0.5
        low = jnp.where(row < 16, deeper[2 * s : 2 * s + 1], deeper[2 * s + 1 : 2 * s + 2])
        tendency = sums[s] + high_ref[s] + jnp.where(target, low, 0.0)
        out_ref[s] = jnp.where(live, tendency, 0.0).astype(bf16)


def stay(*arrays, space=pltpu.HBM):
    return [pltpu.with_memory_space_constraint(x, space) for x in arrays]


def smem():
    return pl.BlockSpec(memory_space=pltpu.SMEM)


def vmem():
    return pl.BlockSpec(memory_space=pltpu.VMEM)


def hbm():
    return pl.BlockSpec(memory_space=pltpu.HBM)


def grid_call(n, got, quad_weight, totals, near):
    all_rows = n.n_wave * n.rows
    signs = np.zeros((8, LANES), np.float32)
    signs[:4] = np.repeat(image_signs(), LANES // IMAGES, axis=1)
    table = pltpu.VMEM((GROUP, n.keys // 2, n.width), f32)
    coef = pltpu.VMEM((GROUP, LANES, n.keys), f32)
    return pl.pallas_call(
        lambda *refs: grid_kernel(n, *refs),
        out_shape=(pltpu.HBM((all_rows, LANES), bf16), pltpu.HBM(totals.shape, f32), pltpu.HBM(totals.shape, f32)),
        in_specs=[vmem()] * 3 + [hbm()] * 2,
        out_specs=(hbm(),) * 3,
        scratch_shapes=[
            pltpu.VMEM((4, n.n_wave * n.rows, LANES), f32),
            table,
            table,
            coef,
            coef,
            pltpu.VMEM((2, n.half, 8, LANES), f32),
            pltpu.VMEM((all_rows, LANES), f32),
            pltpu.VMEM((all_rows, LANES), bf16),
            pltpu.VMEM(totals.shape, f32),
            pltpu.VMEM(totals.shape, f32),
            pltpu.VMEM(totals.shape, f32),
            pltpu.SMEM((n.lats,), f32),
            pltpu.SemaphoreType.DMA,
            pltpu.SemaphoreType.DMA((2,)),
            pltpu.SemaphoreType.DMA((2,)),
            pltpu.VMEM((2, n.half, LANES), f32),
            pltpu.VMEM((2, n.half, LANES), f32),
        ],
        compiler_params=pltpu.CompilerParams(vmem_limit_bytes=24 * 1024 * 1024),
        name="grid_stage",
    )(
        got,
        jnp.asarray(signs),
        near,
        *stay(quad_weight, totals),
    )


def fast_body(n, spec, legendre, layer_depth_share, quad_weight, wave_of_slot):
    params = pltpu.CompilerParams(vmem_limit_bytes=24 * 1024 * 1024)
    all_rows = n.n_wave * n.rows
    dma = pltpu.SemaphoreType.DMA
    held_shape = (2, n.lats + 16, n.span)
    high_shape = (2, n.cols, n.span)
    total_shape = (4, n.span)
    sent, totals, held, high = pl.pallas_call(
        lambda *refs: forward_kernel(n, *refs),
        out_shape=(
            pltpu.HBM((n.n_wave, n.sent, LANES), bf16),
            pltpu.HBM(total_shape, f32),
            pltpu.VMEM(held_shape, bf16),
            pltpu.HBM(high_shape, f32),
        ),
        in_specs=[hbm()] * 4,
        out_specs=(hbm(), hbm(), vmem(), hbm()),
        scratch_shapes=[
            pltpu.SMEM((2,), jnp.int32),
            pltpu.SMEM((n.layers,), f32),
            pltpu.VMEM(spec.shape, bf16),
            pltpu.VMEM(total_shape, f32),
            pltpu.VMEM(high_shape, f32),
            pltpu.VMEM((n.lats, LANES), f32),
            dma((3,)),
            dma((2, 2 * PIECES)),
            dma((3,)),
            pltpu.VMEM((n.n_wave, n.sent, LANES), bf16),
            dma((2,)),
        ],
        compiler_params=params,
        name="legendre_forward",
    )(*stay(wave_of_slot, layer_depth_share, spec, legendre))
    near = lax.ppermute(totals, "lev", [(i, i ^ 1) for i in range(n.n_lev)])
    got = lax.all_to_all(sent, "wave", split_axis=0, concat_axis=0, tiled=True)
    out, pair, keep = grid_call(n, got.reshape(n.n_wave * n.sent, LANES), quad_weight, totals, near)
    far = lax.ppermute(pair, "lev", [(i, i ^ 2) for i in range(n.n_lev)])
    back = lax.all_to_all(
        out.reshape(n.n_wave, n.rows, LANES), "wave", split_axis=0, concat_axis=0, tiled=True
    )
    return pl.pallas_call(
        lambda *refs: back_kernel(n, *refs),
        out_shape=jax.ShapeDtypeStruct(spec.shape, bf16),
        in_specs=[hbm()] * 3 + [vmem()] * 3,
        out_specs=vmem(),
        scratch_shapes=[
            pltpu.VMEM((2, n.circles, LANES), bf16),
            pltpu.VMEM(total_shape, f32),
            pltpu.VMEM(total_shape, f32),
            pltpu.VMEM(high_shape, f32),
            dma((3,)),
        ],
        compiler_params=params,
        name="legendre_back",
    )(
        *stay(far, keep, high),
        back.reshape(all_rows, LANES),
        jnp.asarray(order_matrix(n), bf16),
        *stay(held, space=pltpu.VMEM),
    )


full_turn = 2.0 * math.pi


def carried_in(part, axis, combine, identity):
    count = lax.axis_size(axis)
    place = lax.axis_index(axis)
    ahead = count - 1 - place
    gathered = lax.all_gather(part, axis)
    state = jnp.zeros_like(part) + jnp.asarray(identity, part.dtype)

    def one(hop, state):
        source = count - 1 - hop
        return combine(state, lax.dynamic_index_in_dim(gathered, source, 0, False))

    return lax.fori_loop(0, ahead, one, state)


def rate_bundle(
    eastward_velocity,
    northward_velocity,
    local_curl_spin,
    thermal_state,
    planetary_rotation_effect,
    processor_dimension,
):
    absolute = local_curl_spin + planetary_rotation_effect
    return jnp.stack(
        [
            absolute * eastward_velocity,
            absolute * northward_velocity,
            0.5 * (eastward_velocity * eastward_velocity + northward_velocity * northward_velocity),
            eastward_velocity * thermal_state,
        ],
        axis=processor_dimension,
    )


def row_latitudes(device, per_dev, total_lat):
    row_ids = jnp.arange(per_dev, dtype=jnp.int32)
    quarter = per_dev // 4
    block_ids = row_ids // 4
    hemisphere = row_ids // 2 % 2
    member = row_ids % 2
    first_dist = device * quarter + block_ids
    pole_dist = jnp.where(member == 0, first_dist, total_lat // 2 - 1 - first_dist)
    return jnp.where(hemisphere == 0, pole_dist, total_lat - 1 - pole_dist)


def add_terms(earlier, later):
    return earlier + later


def general_body(spec, legendre, layer_depth_share, quad_weight, wave_of_slot):
    number_of_slots, columns, degree_list = spec.shape
    total_lat = legendre.shape[1]
    groups = lax.axis_size("wave")
    device = lax.axis_index("wave")
    per_dev = total_lat // groups
    layers_on_processor = layer_depth_share.shape[0]
    field_stack = columns // (2 * layers_on_processor)
    flat_rows = field_stack * layers_on_processor
    max_points = 20 + 4 * (total_lat // 2 - 1)
    all_waves = lax.all_gather(wave_of_slot, "wave", axis=0, tiled=True)
    wave_count = all_waves.shape[0]
    weight_two = jnp.where(all_waves == 0, 1.0, 2.0).astype(jnp.float32)
    degree_index = jnp.arange(degree_list, dtype=jnp.int32)
    valid_cols = degree_index[None, :] < (degree_list - wave_of_slot)[:, None]
    screened_entries = jnp.where(valid_cols[:, None, :], spec, jnp.zeros_like(spec))
    thermal_state = screened_entries.reshape(
        number_of_slots, 2, field_stack, layers_on_processor, degree_list
    )[:, :, 3].astype(jnp.float32)
    scaled_entries = thermal_state * layer_depth_share[None, None, :, None]
    below_sum = jnp.flip(jnp.cumsum(jnp.flip(scaled_entries, 2), 2), 2)
    deeper = carried_in(
        below_sum[:, :, 0],
        "lev",
        add_terms,
        jnp.zeros((number_of_slots, 2, degree_list), jnp.float32),
    )
    geopot = below_sum + deeper[:, :, None, :]
    fourier = jnp.einsum(
        "sln,scn->lsc", legendre, screened_entries, preferred_element_type=jnp.float32
    ).astype(jnp.bfloat16)
    send_order = row_latitudes(
        jnp.arange(groups, dtype=jnp.int32)[:, None], per_dev, total_lat
    ).reshape(-1)
    send_rows = jnp.take(fourier, send_order, axis=0).reshape(total_lat, number_of_slots * columns)
    received = lax.all_to_all(send_rows, "wave", split_axis=0, concat_axis=1, tiled=True)
    coeffs = received.reshape(per_dev, wave_count, 2, flat_rows)
    latitudes = row_latitudes(device, per_dev, total_lat)
    lengths = 20 + 4 * jnp.minimum(latitudes, total_lat - 1 - latitudes)
    planetary_rotation_effect = 2.0 * jnp.cos(
        (latitudes.astype(jnp.float32) + 0.5) * (math.pi / total_lat)
    )
    row_scale = quad_weight[latitudes] / lengths.astype(jnp.float32)
    quarter = per_dev // 4
    pair_points = max_points + 20
    tile_count = -(-pair_points // 128)
    padded = tile_count * 128
    pair_len = lengths.reshape(quarter, 2, 2)[:, 0, :]
    first_len = pair_len[:, 0:1]
    second_len = pair_len[:, 1:2]
    points = jnp.arange(padded, dtype=jnp.int32)[None, :]
    first_lat = points < first_len
    in_pair = points < pair_points
    local_idx = jnp.where(first_lat, points, points - first_len)
    point_len = jnp.where(first_lat, first_len, second_len)
    phase_int = all_waves[None, :, None] * local_idx[:, None, :] % point_len[:, None, :]
    angles = phase_int.astype(jnp.float32) * full_turn / point_len.astype(jnp.float32)[:, None, :]
    cosine = jnp.cos(angles)
    sine_vals = jnp.sin(angles)
    resolved = (2 * all_waves[None, :, None] < point_len[:, None, :]) & in_pair[:, None, :]
    amplitude = jnp.where(resolved, weight_two[None, :, None], 0.0)
    forward_tab = jnp.concatenate([amplitude * cosine, -(amplitude * sine_vals)], 1).astype(
        jnp.bfloat16
    )
    back_tab = jnp.concatenate(
        [jnp.where(resolved, cosine, 0.0), -jnp.where(resolved, sine_vals, 0.0)], 1
    ).astype(jnp.bfloat16)
    forward_tiles = forward_tab.reshape(quarter, 2 * wave_count, tile_count, 128)
    back_tiles = back_tab.reshape(quarter, 2 * wave_count, tile_count, 128)
    tile_start = jnp.arange(tile_count, dtype=jnp.int32)[None, :] * 128
    owner_second = tile_start + 128 > first_len
    boundary = first_len[:, 0] // 128
    is_bound = jnp.arange(tile_count, dtype=jnp.int32)[None, :] == boundary[:, None]
    first_tiles = first_lat.reshape(quarter, tile_count, 128)
    stacked = coeffs.reshape(quarter, 2, 2, wave_count, 2, flat_rows).transpose(0, 1, 2, 4, 3, 5)
    stacked = stacked.reshape(quarter, 2, 2, 2 * wave_count, flat_rows)
    coef_tiles = jnp.where(
        owner_second[:, None, :, None, None],
        stacked[:, :, 1][:, :, None],
        stacked[:, :, 0][:, :, None],
    )
    grid_tiles = jnp.einsum(
        "qatkf,qktp->qaftp", coef_tiles, forward_tiles, preferred_element_type=jnp.float32
    )
    bound_fwd = jnp.take_along_axis(forward_tiles, boundary[:, None, None, None], axis=2)[:, :, 0]
    bound_back = jnp.take_along_axis(back_tiles, boundary[:, None, None, None], axis=2)[:, :, 0]
    edge_grid = jnp.einsum(
        "qakf,qkp->qafp", stacked[:, :, 0], bound_fwd, preferred_element_type=jnp.float32
    )
    use_edge = is_bound[:, :, None] & first_tiles
    grid_tiles = jnp.where(use_edge[:, None, None], edge_grid[:, :, :, None, :], grid_tiles)
    grid_vals = grid_tiles.reshape(quarter, 2, field_stack, layers_on_processor, padded)
    row_cor = planetary_rotation_effect.reshape(quarter, 2, 2)
    point_cor = jnp.where(first_lat[:, None, :], row_cor[:, :, 0:1], row_cor[:, :, 1:2])[
        :, :, None, :
    ]
    products = rate_bundle(
        grid_vals[:, :, 0], grid_vals[:, :, 1], grid_vals[:, :, 2], grid_vals[:, :, 3], point_cor, 2
    )
    products = products.astype(jnp.bfloat16).reshape(quarter, 2, flat_rows, tile_count, 128)
    keep = jnp.where(owner_second[:, :, None], jnp.logical_not(first_tiles), first_tiles)
    main_prods = jnp.where(keep[:, None, None], products, jnp.zeros_like(products))
    per_tile = jnp.einsum(
        "qaftp,qktp->qatkf", main_prods, back_tiles, preferred_element_type=jnp.float32
    )
    bound_prods = jnp.take_along_axis(products, boundary[:, None, None, None, None], axis=3)[
        :, :, :, 0
    ]
    bound_first = jnp.take_along_axis(first_tiles, boundary[:, None, None], axis=1)[:, 0]
    bound_prods = jnp.where(bound_first[:, None, None, :], bound_prods, jnp.zeros_like(bound_prods))
    edge_back = jnp.einsum(
        "qafp,qkp->qakf", bound_prods, bound_back, preferred_element_type=jnp.float32
    )
    owner_mask = owner_second[:, None, :, None, None]
    first_ret = jnp.sum(jnp.where(owner_mask, 0.0, per_tile), axis=2) + edge_back
    second_ret = jnp.sum(jnp.where(owner_mask, per_tile, 0.0), axis=2)
    returned = jnp.stack([first_ret, second_ret], axis=2)
    returned = (returned * row_scale.reshape(quarter, 2, 2)[:, :, :, None, None]).astype(
        jnp.bfloat16
    )
    out_rows = returned.reshape(quarter, 2, 2, 2, wave_count, flat_rows).transpose(0, 1, 2, 4, 3, 5)
    out_rows = out_rows.reshape(per_dev, wave_count * columns)
    gathered_rows = lax.all_to_all(out_rows, "wave", split_axis=1, concat_axis=0, tiled=True)
    inverse = (
        jnp.zeros((total_lat,), jnp.int32)
        .at[send_order]
        .set(jnp.arange(total_lat, dtype=jnp.int32))
    )
    back_fourier = jnp.take(gathered_rows, inverse, axis=0).reshape(
        total_lat, number_of_slots, columns
    )
    tendency = jnp.einsum(
        "lsc,sln->scn", back_fourier, legendre, preferred_element_type=jnp.float32
    )
    tendency = tendency.reshape(number_of_slots, 2, field_stack, layers_on_processor, degree_list)
    tendency = tendency.at[:, :, 2].add(geopot)
    tendency = jnp.where(valid_cols[:, None, None, None, :], tendency, 0.0)
    return tendency.reshape(number_of_slots, columns, degree_list).astype(jnp.bfloat16)


def solution(mesh):
    def body(spec, legendre, layer_depth_share, quad_weight, wave_of_slot):
        slots, cols, span = spec.shape
        layers = layer_depth_share.shape[0]
        n = Sizes(mesh.shape["wave"], mesh.shape["lev"], slots, cols, legendre.shape[1], span, layers)
        step = (lambda *args: fast_body(n, *args)) if n.fits() else general_body
        return step(spec, legendre, layer_depth_share, quad_weight, wave_of_slot)

    in_specs = (P("wave", "lev", None), P("wave", None, None), P("lev"), P(), P("wave"))
    out_specs = P("wave", "lev", None)
    return jax.shard_map(body, mesh=mesh, in_specs=in_specs, out_specs=out_specs, check_vma=False)
```

```python
import math

import numpy as np
import jax
import jax.numpy as jnp
from jax import lax
from jax.experimental import pallas as pl
from jax.experimental.pallas import tpu as pltpu
from jax.sharding import PartitionSpec as P

bf16 = jnp.bfloat16
f32 = jnp.float32
FIELDS = 4
IMAGES = 4
LANES = 128
ROUNDER = 12582912.0
CHUNK = 256
GROUP = 2
PIECES = 2
FLIGHT = 2


def nt(a, b):
    return lax.dot_general(a, b, (((1,), (1,)), ((), ())), preferred_element_type=f32)


def nn(a, b):
    return lax.dot_general(a, b, (((1,), (0,)), ((), ())), preferred_element_type=f32)


def circle_polynomials():
    f = np.cos(np.pi * (np.arange(4000) + 0.5) / 8000) * 0.505
    z = f * f
    out = []
    for values in (np.cos(np.pi * f), np.sin(np.pi * f) / f):
        fit = np.polynomial.chebyshev.Chebyshev.fit(z, math.sqrt(2.0) * values, 4, domain=[0, 0.2551])
        out.append([float(c) for c in fit.convert(kind=np.polynomial.Polynomial).coef])
    return out


COS_POLY, SIN_POLY = circle_polynomials()


def horner(z, coefs):
    acc = z * coefs[-1] + coefs[-2]
    for c in coefs[-3::-1]:
        acc = acc * z + c
    return acc


def cos_sin(count, length, inverse):
    turns = (count * inverse + ROUNDER) - ROUNDER
    f = (count - turns * length) * inverse
    z = f * f
    half_sin = f * horner(z, SIN_POLY)
    return 1.0 - half_sin * half_sin, half_sin * horner(z, COS_POLY)


def image_signs():
    return np.array([[1, 1, 1, 1], [-1, 1, -1, 1], [1, 1, -1, -1], [-1, 1, 1, -1]], np.float32)


class Sizes:
    def __init__(self, n_wave, n_lev, slots, cols, lats, span, layers):
        self.n_wave, self.n_lev, self.slots, self.cols = n_wave, n_lev, slots, cols
        self.lats, self.span, self.layers = lats, span, layers
        self.rows = lats // n_wave // 2
        self.half = self.rows // 2
        self.circles = lats // 2
        self.points = self.circles + 11
        self.width = -(-self.points // CHUNK) * CHUNK
        self.tiles = self.width // LANES
        self.sent = self.rows + 8
        self.keys = 8 * n_wave

    def fits(self):
        return (
            self.slots == 2
            and self.cols == 32
            and self.layers == 4
            and self.n_wave == 8
            and self.n_lev == 4
            and self.rows % 16 == 0
            and self.half % GROUP == 0
            and self.half % 8 == 0
            and self.half * 4 * self.n_wave == self.lats
            and self.span % LANES == 0
            and (self.n_wave * self.rows) % LANES == 0
            and self.tiles <= 8
        )

    def block_starts(self, owner):
        h = self.half
        return (
            (h * owner, self.circles - h * (owner + 1)),
            (self.lats - h * (owner + 1), self.circles + h * owner),
        )


def order_matrix(n):
    out = np.zeros((LANES, LANES), np.float32)
    for parity in range(2):
        for part in range(2):
            for hemi in range(2):
                for field in range(FIELDS):
                    for layer in range(n.layers):
                        row = hemi * 64 + parity * 32 + part * 16 + field * 4 + layer
                        lane = (parity * 2 + part) * 32 + field * 8 + hemi * 4 + layer
                        out[row, lane] = 1.0
    return out


def live_spec(n, spec, wave):
    degree = lax.broadcasted_iota(jnp.int32, (n.cols, n.span), 1)
    live = degree < n.span - wave
    return jnp.where(live, spec.astype(f32), 0.0), live


def layer_sums(n, masked, share_ref):
    row = lax.broadcasted_iota(jnp.int32, (n.cols, n.span), 0)
    layer = row % n.layers
    weight = jnp.where(
        layer < 2,
        jnp.where(layer == 0, share_ref[0], share_ref[1]),
        jnp.where(layer == 2, share_ref[2], share_ref[3]),
    )
    warm = (row // n.layers) % FIELDS == FIELDS - 1
    y = jnp.where(warm, masked * weight, 0.0)
    y = y + pltpu.roll(y, n.cols - 1, 0)
    return y + pltpu.roll(y, n.cols - 2, 0)


def fetch(pairs, sems):
    copies = [pltpu.make_async_copy(src, dst, sems.at[k]) for k, (src, dst) in enumerate(pairs)]
    for copy in copies:
        copy.start()
    return copies


def forward_kernel(n, wave_hbm, share_hbm, spec_hbm, leg_hbm, out_hbm, total_hbm, leg, high_hbm, wave_ref, share_ref, spec_ref, total_ref, high_ref, acc, sems, leg_sems, done_sems, out_ref, out_sems):
    small = fetch(((wave_hbm, wave_ref), (share_hbm, share_ref), (spec_hbm, spec_ref)), sems)
    size = n.circles // PIECES
    big = [
        [
            pltpu.make_async_copy(leg_hbm.at[s, pl.ds(k * size, size), :], leg.at[s, pl.ds(k * size, size), :], leg_sems.at[s, k])
            for s in range(2)
        ]
        for k in range(2 * PIECES)
    ]
    for pair in big[:FLIGHT]:
        for copy in pair:
            copy.start()
    for copy in small:
        copy.wait()
    row = lax.broadcasted_iota(jnp.int32, (n.cols, n.span), 0)
    target = (row // n.layers) % FIELDS == 2
    tables = [[], []]
    for s in range(2):
        masked, live = live_spec(n, spec_ref[s], wave_ref[s])
        sums = layer_sums(n, masked, share_ref)
        for part in range(2):
            total_ref[2 * s + part : 2 * s + part + 1, :] = sums[part * 16 + 12 : part * 16 + 13, :]
        high_ref[s] = jnp.where(target, pltpu.roll(sums, n.cols - n.layers, 0), 0.0)
        leg[s, n.lats : n.lats + 8, :] = jnp.where(live[:8], 1.0, 0.0).astype(bf16)
        leg[s, n.lats + 8 : n.lats + 16, :] = jnp.full((8, n.span), (1 - wave_ref[s] % 2).astype(f32)).astype(bf16)
        scaled = masked * jnp.where(wave_ref[s] == 0, 1.0, 2.0)
        none = jnp.zeros_like(scaled[:16])
        for hemi in range(2):
            rows = []
            for parity in range(2):
                mine = wave_ref[s] % 2 == parity
                for part in range(2):
                    chunk = jnp.where(mine, scaled[part * 16 : part * 16 + 16], 0.0)
                    rows += [chunk, none] if hemi == 0 else [none, chunk]
            tables[hemi].append(jnp.concatenate(rows, 0).astype(bf16))
    tables = [jnp.concatenate(pair, 1) for pair in tables]
    even = jnp.where(wave_ref[0] % 2 == 0, wave_ref[0], wave_ref[1])
    lane = lax.broadcasted_iota(jnp.int32, (8, LANES), 1)
    tag = jnp.where(lane < LANES // 2, even // 16, even % 16).astype(f32).astype(bf16)
    for owner in range(n.n_wave):
        out_ref[owner, n.rows : n.sent, :] = tag

    def strip(start, count):
        return out_ref.at[:, pl.ds(start, count), :], out_hbm.at[:, pl.ds(start, count), :]

    leaving = fetch(((total_ref, total_hbm), (high_ref, high_hbm), strip(n.rows, 8)), done_sems)
    for k in range(2 * PIECES):
        for copy in big[k]:
            copy.wait()
        if k + FLIGHT < 2 * PIECES:
            for copy in big[k + FLIGHT]:
                copy.start()
        rows = slice(k * size, (k + 1) * size)
        both = jnp.concatenate([leg[0, rows, :], leg[1, rows, :]], 1)
        acc[rows, :] = nt(both, tables[k // PIECES])
        if k >= PIECES and (k + 1) % (PIECES // 2) == 0:
            b = 3 - (k + 1) // (PIECES // 2) + 1
            for owner in range(n.n_wave):
                starts = n.block_starts(owner)
                block = acc[starts[0][b] : starts[0][b] + n.half, :] + acc[starts[1][b] : starts[1][b] + n.half, :]
                out_ref[owner, b * n.half : (b + 1) * n.half, :] = block.astype(bf16)
            copy = pltpu.make_async_copy(*strip(b * n.half, n.half), out_sems.at[b])
            copy.start()
            leaving.append(copy)
    for copy in leaving:
        copy.wait()


def grid_kernel(n, got_ref, sign_ref, near_ref, quad_hbm, total_hbm, out_hbm, pair_hbm, keep_hbm, spread, table_a, table_b, coef_a, coef_b, rows, out, total_ref, pair_ref, keep_ref, quad_ref, out_sem, in_sems, side_sems, inv_ref, cor_ref):
    arriving = fetch(((quad_hbm, quad_ref), (total_hbm, total_ref)), in_sems)
    device = lax.axis_index("wave")
    first_circle = device * n.half
    top = n.span - 1
    lane = lax.broadcasted_iota(jnp.int32, (8, LANES), 1)
    lane_f = lane.astype(f32)
    north = (lane // 4) % 2 == 0
    sent_lane = lax.broadcasted_iota(jnp.int32, (LANES, LANES), 0)
    to = lax.broadcasted_iota(jnp.int32, (LANES, LANES), 1)
    source = (to // 4 % 2) * 16 + (to // 8 % FIELDS) * 4 + to % 4
    for p in range(4):
        pick = jnp.where(sent_lane == source + p * 32, sign_ref[p : p + 1, :], 0.0).astype(bf16)
        wide = nn(got_ref[...], pick)
        for src in range(n.n_wave):
            for r in range(0, n.rows, 8):
                spread[p, pl.ds(r * n.n_wave + src, 8, stride=n.n_wave), :] = wide[src * n.sent + r : src * n.sent + r + 8]
    raw = got_rows_f32(n, got_ref)
    tag = jnp.where(lane < LANES // 2, raw * 16.0, raw)
    even_m = tag + pltpu.roll(tag, LANES // 2, 1)
    odd_m = float(top) - even_m
    even_2 = 2.0 * even_m
    odd_2 = 2.0 * odd_m
    for k in range(2):
        step = lax.broadcasted_iota(jnp.int32, (n.half, LANES), 0)
        circle = first_circle + step if k == 0 else n.circles - 1 - first_circle - step
        inv_ref[k] = 1.0 / (20 + 4 * circle).astype(f32)
        whole = jnp.full((n.half, LANES), 4.0 * n.lats, f32)
        cosine, _ = cos_sin((2 * circle + 1).astype(f32), whole, 1.0 / (4 * n.lats))
        cor_ref[k] = 2.0 * cosine
    tile_point = (lax.broadcasted_iota(jnp.int32, (8, LANES), 0) * LANES + lane).astype(f32)

    def sizes(i):
        short = first_circle + i
        return short, n.circles - 1 - short

    def build(i, u, table):
        short, long = sizes(i)
        cut = (short + 6).astype(f32)
        len_s = (20 + 4 * short).astype(f32)
        len_l = (20 + 4 * long).astype(f32)
        inv_s = inv_ref[0, pl.ds(i, 1), :]
        inv_l = inv_ref[1, pl.ds(i, 1), :]

        def places(point):
            own = point < cut
            return jnp.where(own, point, point - cut), jnp.where(own, len_s, len_l), jnp.where(own, inv_s, inv_l)

        j, length, inverse = places(tile_point)
        top_c, top_s = cos_sin(j * float(top), length, inverse)
        for t in range(n.tiles):
            j, length, inverse = places(lane_f + float(t * LANES))
            c, s = cos_sin(even_m * j, length, inverse)
            tc = jnp.broadcast_to(top_c[t : t + 1, :], (8, LANES))
            ts = jnp.broadcast_to(top_s[t : t + 1, :], (8, LANES))
            span = slice(t * LANES, (t + 1) * LANES)
            table[u, 0:8, span] = c
            table[u, 8:16, span] = s
            table[u, 16:24, span] = tc * c + ts * s
            table[u, 24:32, span] = ts * c - tc * s

    def gather(i, u, coef):
        short, long = sizes(i)
        parts = []
        for circle, row_n, row_s in (
            (short, i, n.half - 1 - i),
            (long, n.rows - 1 - i, n.half + i),
        ):
            length = (20 + 4 * circle).astype(f32)
            for p in range(4):
                up = spread[p, pl.ds(row_n * 8, 8), :]
                down = spread[p, pl.ds(row_s * 8, 8), :]
                seen = (odd_2 if p > 1 else even_2) < length
                parts.append(jnp.where(seen, jnp.where(north, up, down), 0.0))
        coef[u] = jnp.transpose(jnp.concatenate(parts, 0))

    south = lax.broadcasted_iota(jnp.int32, (8, LANES), 0) // 4
    lane_b = lax.broadcasted_iota(jnp.int32, (16, LANES), 1).astype(f32).astype(bf16)
    signs = [sign_ref[p : p + 1, :] for p in range(4)]
    group = lane // 32
    kinetic = jnp.where((lane // 8) % FIELDS == 2, 0.5, 1.0)

    def weights(t, cut):
        edge_at = jnp.clip(cut - t * LANES, -4, LANES + 4).astype(f32) - 0.5
        x = jnp.full((16, LANES), edge_at, f32).astype(bf16) - lane_b
        share = jnp.minimum(jnp.abs(x), 1.0)
        own = jnp.minimum(jnp.maximum(x + 0.5, 0.0), 1.0)
        if t == 0 or (t + 1) * LANES >= n.points:
            point = lax.broadcasted_iota(jnp.int32, (16, LANES), 1) + t * LANES
            ends = (point == 0) | (point == n.points - 1)
            share = share * jnp.where(ends, 0.5, jnp.where(point < n.points, 1.0, 0.0)).astype(bf16)
        own_share = own * share
        return own, 1.0 - own, own_share, share - own_share

    def transform(i, u, table, coef):
        short, long = sizes(i)
        cut = short + 6
        left = coef[u].astype(bf16)
        cor_s = cor_ref[0, pl.ds(i, 1), :]
        cor_l = cor_ref[1, pl.ds(i, 1), :]
        total = None
        for c in range(n.width // CHUNK):
            ahead, behind, spins = [], [], []
            for t in range(c * CHUNK // LANES, (c + 1) * CHUNK // LANES):
                tab = table[u, :, t * LANES : (t + 1) * LANES].astype(bf16)
                own, rest, own_share, rest_share = weights(t, cut)
                ahead.append(jnp.concatenate([tab[:16] * own, tab[16:] * own, tab[:16] * rest, tab[16:] * rest], 0))
                behind.append(
                    jnp.concatenate(
                        [tab[:16] * own_share, tab[16:] * own_share, tab[:16] * rest_share, tab[16:] * rest_share], 0
                    )
                )
                spin = jnp.where(lane < cut - t * LANES, cor_s, cor_l)
                spins.append(jnp.where(south == 0, spin, -spin))
            grid = nn(left, jnp.concatenate(ahead, 1)).reshape(IMAGES, FIELDS, 8, CHUNK)
            x, y, curl, warm = grid[:, 0], grid[:, 1], grid[:, 2], grid[:, 3]
            absolute = curl + jnp.concatenate(spins, 1)
            prods = jnp.stack([absolute * x, absolute * y, x * x + y * y, x * warm], 1)
            piece = nt(jnp.concatenate(behind, 1), prods.reshape(LANES, CHUNK).astype(bf16))
            total = piece if total is None else total + piece
        results = []
        for k, circle in enumerate((short, long)):
            length = (20 + 4 * circle).astype(f32)
            folded = None
            for p in range(4):
                y = total[(4 * k + p) * 8 : (4 * k + p + 1) * 8] * signs[p]
                y = y + pltpu.roll(y, 64, 1)
                y = y + pltpu.roll(y, 32, 1)
                y = jnp.where((odd_2 if p > 1 else even_2) < length, y, 0.0)
                folded = y if folded is None else jnp.where(group == p, y, folded)
            weight = jnp.where(north, quad_ref[circle], quad_ref[n.lats - 1 - circle])
            results.append(folded * (weight * (inv_ref[k, pl.ds(i, 1), :] * kinetic)))
        return results

    turns = [i for k in range(n.half // 2) for i in (k, n.half - 1 - k)]
    groups = [turns[k : k + GROUP] for k in range(0, n.half, GROUP)]

    def ready(members, table, coef):
        for u, i in enumerate(members):
            build(i, u, table)
            gather(i, u, coef)

    def work(members, table, coef):
        for u in range(0, GROUP, 2):
            i, other = members[u : u + 2]
            short_i, long_i = transform(i, u, table, coef)
            short_o, long_o = transform(other, u + 1, table, coef)
            for at, up, down in (
                (i, short_i, short_o),
                (other, short_o, short_i),
                (n.half + i, long_o, long_i),
                (n.half + other, long_i, long_o),
            ):
                rows[pl.ds(at, 8, stride=n.rows), :] = jnp.where(north, up, down)

    ready(groups[0], table_a, coef_a)
    for copy in arriving:
        copy.wait()
    pair_ref[...] = total_ref[...] + near_ref[...]
    keep_ref[...] = jnp.where(lax.axis_index("lev") % 2 == 0, near_ref[...], 0.0)
    leaving = fetch(((pair_ref, pair_hbm), (keep_ref, keep_hbm)), side_sems)
    buffers = ((table_a, coef_a), (table_b, coef_b))
    for k, members in enumerate(groups):
        if k + 1 < len(groups):
            ready(groups[k + 1], *buffers[(k + 1) % 2])
        work(members, *buffers[k % 2])

    out[...] = rows[...].astype(bf16)
    copy = pltpu.make_async_copy(out, out_hbm, out_sem)
    copy.start()
    for side in leaving:
        side.wait()
    copy.wait()


def got_rows_f32(n, got_ref):
    pieces = [got_ref[src * n.sent + n.rows : src * n.sent + n.rows + 8, :].astype(f32)[:1] for src in range(n.n_wave)]
    return jnp.concatenate(pieces, 0)


def back_kernel(n, far_hbm, keep_hbm, high_hbm, back_ref, order_ref, leg, out_ref, turn, far_ref, keep_ref, high_ref, sems):
    arriving = fetch(((far_hbm, far_ref), (keep_hbm, keep_ref), (high_hbm, high_ref)), sems)
    for owner in range(n.n_wave):
        starts = n.block_starts(owner)
        for b in range(2):
            block = back_ref[owner * n.rows + b * n.half : owner * n.rows + (b + 1) * n.half, :]
            for hemi in range(2):
                at = starts[hemi][b] - hemi * n.circles
                turn[hemi, at : at + n.half, :] = block
    turned = [nt(order_ref[hemi * 64 : hemi * 64 + 64, :], turn[hemi]) for hemi in range(2)]
    row = lax.broadcasted_iota(jnp.int32, (n.cols, n.span), 0)
    target = (row // n.layers) % FIELDS == 2
    sums = []
    for s in range(2):
        even = leg[s, n.lats + 8 : n.lats + 16, :].astype(f32)[:1] > 0.5
        for hemi in range(2):
            mine = jnp.where(even, turned[hemi][:32], turned[hemi][32:]).astype(bf16)
            piece = nn(mine, leg[s, hemi * n.circles : (hemi + 1) * n.circles, :])
            sums.append(piece if hemi == 0 else sums.pop() + piece)
    for copy in arriving:
        copy.wait()
    deeper = keep_ref[...] + jnp.where(lax.axis_index("lev") < n.n_lev // 2, far_ref[...], 0.0)
    for s in range(2):
        live = leg[s, n.lats : n.lats + 8, :].astype(f32)[:1] > 0.5
        low = jnp.where(row < 16, deeper[2 * s : 2 * s + 1], deeper[2 * s + 1 : 2 * s + 2])
        tendency = sums[s] + high_ref[s] + jnp.where(target, low, 0.0)
        out_ref[s] = jnp.where(live, tendency, 0.0).astype(bf16)


def stay(*arrays, space=pltpu.HBM):
    return [pltpu.with_memory_space_constraint(x, space) for x in arrays]


def kernel_params():
    return pltpu.CompilerParams(
        vmem_limit_bytes=24 * 1024 * 1024
    )


def smem():
    return pl.BlockSpec(memory_space=pltpu.SMEM)


def vmem():
    return pl.BlockSpec(memory_space=pltpu.VMEM)


def hbm():
    return pl.BlockSpec(memory_space=pltpu.HBM)


def grid_call(n, got, quad_weight, totals, near):
    all_rows = n.n_wave * n.rows
    signs = np.zeros((8, LANES), np.float32)
    signs[:4] = np.repeat(image_signs(), LANES // IMAGES, axis=1)
    table = pltpu.VMEM((GROUP, n.keys // 2, n.width), f32)
    coef = pltpu.VMEM((GROUP, LANES, n.keys), f32)
    return pl.pallas_call(
        lambda *refs: grid_kernel(n, *refs),
        out_shape=(pltpu.HBM((all_rows, LANES), bf16), pltpu.HBM(totals.shape, f32), pltpu.HBM(totals.shape, f32)),
        in_specs=[vmem()] * 3 + [hbm()] * 2,
        out_specs=(hbm(),) * 3,
        scratch_shapes=[
            pltpu.VMEM((4, n.n_wave * n.rows, LANES), f32),
            table,
            table,
            coef,
            coef,
            pltpu.VMEM((all_rows, LANES), f32),
            pltpu.VMEM((all_rows, LANES), bf16),
            pltpu.VMEM(totals.shape, f32),
            pltpu.VMEM(totals.shape, f32),
            pltpu.VMEM(totals.shape, f32),
            pltpu.SMEM((n.lats,), f32),
            pltpu.SemaphoreType.DMA,
            pltpu.SemaphoreType.DMA((2,)),
            pltpu.SemaphoreType.DMA((2,)),
            pltpu.VMEM((2, n.half, LANES), f32),
            pltpu.VMEM((2, n.half, LANES), f32),
        ],
        compiler_params=kernel_params(),
        name="grid_stage",
    )(
        got,
        jnp.asarray(signs),
        near,
        *stay(quad_weight, totals),
    )


def fast_body(n, spec, legendre, layer_depth_share, quad_weight, wave_of_slot):
    params = kernel_params()
    all_rows = n.n_wave * n.rows
    dma = pltpu.SemaphoreType.DMA
    held_shape = (2, n.lats + 16, n.span)
    high_shape = (2, n.cols, n.span)
    total_shape = (4, n.span)
    sent, totals, held, high = pl.pallas_call(
        lambda *refs: forward_kernel(n, *refs),
        out_shape=(
            pltpu.HBM((n.n_wave, n.sent, LANES), bf16),
            pltpu.HBM(total_shape, f32),
            pltpu.VMEM(held_shape, bf16),
            pltpu.HBM(high_shape, f32),
        ),
        in_specs=[hbm()] * 4,
        out_specs=(hbm(), hbm(), vmem(), hbm()),
        scratch_shapes=[
            pltpu.SMEM((2,), jnp.int32),
            pltpu.SMEM((n.layers,), f32),
            pltpu.VMEM(spec.shape, bf16),
            pltpu.VMEM(total_shape, f32),
            pltpu.VMEM(high_shape, f32),
            pltpu.VMEM((n.lats, LANES), f32),
            dma((3,)),
            dma((2, 2 * PIECES)),
            dma((3,)),
            pltpu.VMEM((n.n_wave, n.sent, LANES), bf16),
            dma((2,)),
        ],
        compiler_params=params,
        name="legendre_forward",
    )(*stay(wave_of_slot, layer_depth_share, spec, legendre))
    near = lax.ppermute(totals, "lev", [(i, i ^ 1) for i in range(n.n_lev)])
    got = lax.all_to_all(sent, "wave", split_axis=0, concat_axis=0, tiled=True)
    out, pair, keep = grid_call(n, got.reshape(n.n_wave * n.sent, LANES), quad_weight, totals, near)
    far = lax.ppermute(pair, "lev", [(i, i ^ 2) for i in range(n.n_lev)])
    back = lax.all_to_all(
        out.reshape(n.n_wave, n.rows, LANES), "wave", split_axis=0, concat_axis=0, tiled=True
    )
    return pl.pallas_call(
        lambda *refs: back_kernel(n, *refs),
        out_shape=jax.ShapeDtypeStruct(spec.shape, bf16),
        in_specs=[hbm()] * 3 + [vmem()] * 3,
        out_specs=vmem(),
        scratch_shapes=[
            pltpu.VMEM((2, n.circles, LANES), bf16),
            pltpu.VMEM(total_shape, f32),
            pltpu.VMEM(total_shape, f32),
            pltpu.VMEM(high_shape, f32),
            dma((3,)),
        ],
        compiler_params=params,
        name="legendre_back",
    )(
        *stay(far, keep, high),
        back.reshape(all_rows, LANES),
        jnp.asarray(order_matrix(n), bf16),
        *stay(held, space=pltpu.VMEM),
    )


full_turn = 2.0 * math.pi


def carried_in(part, axis, combine, identity):
    count = lax.axis_size(axis)
    place = lax.axis_index(axis)
    ahead = count - 1 - place
    gathered = lax.all_gather(part, axis)
    state = jnp.zeros_like(part) + jnp.asarray(identity, part.dtype)

    def one(hop, state):
        source = count - 1 - hop
        return combine(state, lax.dynamic_index_in_dim(gathered, source, 0, False))

    return lax.fori_loop(0, ahead, one, state)


def rate_bundle(
    eastward_velocity,
    northward_velocity,
    local_curl_spin,
    thermal_state,
    planetary_rotation_effect,
    processor_dimension,
):
    absolute = local_curl_spin + planetary_rotation_effect
    return jnp.stack(
        [
            absolute * eastward_velocity,
            absolute * northward_velocity,
            0.5 * (eastward_velocity * eastward_velocity + northward_velocity * northward_velocity),
            eastward_velocity * thermal_state,
        ],
        axis=processor_dimension,
    )


def row_latitudes(device, per_dev, total_lat):
    row_ids = jnp.arange(per_dev, dtype=jnp.int32)
    quarter = per_dev // 4
    block_ids = row_ids // 4
    hemisphere = row_ids // 2 % 2
    member = row_ids % 2
    first_dist = device * quarter + block_ids
    pole_dist = jnp.where(member == 0, first_dist, total_lat // 2 - 1 - first_dist)
    return jnp.where(hemisphere == 0, pole_dist, total_lat - 1 - pole_dist)


def add_terms(earlier, later):
    return earlier + later


def general_body(spec, legendre, layer_depth_share, quad_weight, wave_of_slot):
    number_of_slots, columns, degree_list = spec.shape
    total_lat = legendre.shape[1]
    groups = lax.axis_size("wave")
    device = lax.axis_index("wave")
    per_dev = total_lat // groups
    layers_on_processor = layer_depth_share.shape[0]
    field_stack = columns // (2 * layers_on_processor)
    flat_rows = field_stack * layers_on_processor
    max_points = 20 + 4 * (total_lat // 2 - 1)
    all_waves = lax.all_gather(wave_of_slot, "wave", axis=0, tiled=True)
    wave_count = all_waves.shape[0]
    weight_two = jnp.where(all_waves == 0, 1.0, 2.0).astype(jnp.float32)
    degree_index = jnp.arange(degree_list, dtype=jnp.int32)
    valid_cols = degree_index[None, :] < (degree_list - wave_of_slot)[:, None]
    screened_entries = jnp.where(valid_cols[:, None, :], spec, jnp.zeros_like(spec))
    thermal_state = screened_entries.reshape(
        number_of_slots, 2, field_stack, layers_on_processor, degree_list
    )[:, :, 3].astype(jnp.float32)
    scaled_entries = thermal_state * layer_depth_share[None, None, :, None]
    below_sum = jnp.flip(jnp.cumsum(jnp.flip(scaled_entries, 2), 2), 2)
    deeper = carried_in(
        below_sum[:, :, 0],
        "lev",
        add_terms,
        jnp.zeros((number_of_slots, 2, degree_list), jnp.float32),
    )
    geopot = below_sum + deeper[:, :, None, :]
    fourier = jnp.einsum(
        "sln,scn->lsc", legendre, screened_entries, preferred_element_type=jnp.float32
    ).astype(jnp.bfloat16)
    send_order = row_latitudes(
        jnp.arange(groups, dtype=jnp.int32)[:, None], per_dev, total_lat
    ).reshape(-1)
    send_rows = jnp.take(fourier, send_order, axis=0).reshape(total_lat, number_of_slots * columns)
    received = lax.all_to_all(send_rows, "wave", split_axis=0, concat_axis=1, tiled=True)
    coeffs = received.reshape(per_dev, wave_count, 2, flat_rows)
    latitudes = row_latitudes(device, per_dev, total_lat)
    lengths = 20 + 4 * jnp.minimum(latitudes, total_lat - 1 - latitudes)
    planetary_rotation_effect = 2.0 * jnp.cos(
        (latitudes.astype(jnp.float32) + 0.5) * (math.pi / total_lat)
    )
    row_scale = quad_weight[latitudes] / lengths.astype(jnp.float32)
    quarter = per_dev // 4
    pair_points = max_points + 20
    tile_count = -(-pair_points // 128)
    padded = tile_count * 128
    pair_len = lengths.reshape(quarter, 2, 2)[:, 0, :]
    first_len = pair_len[:, 0:1]
    second_len = pair_len[:, 1:2]
    points = jnp.arange(padded, dtype=jnp.int32)[None, :]
    first_lat = points < first_len
    in_pair = points < pair_points
    local_idx = jnp.where(first_lat, points, points - first_len)
    point_len = jnp.where(first_lat, first_len, second_len)
    phase_int = all_waves[None, :, None] * local_idx[:, None, :] % point_len[:, None, :]
    angles = phase_int.astype(jnp.float32) * full_turn / point_len.astype(jnp.float32)[:, None, :]
    cosine = jnp.cos(angles)
    sine_vals = jnp.sin(angles)
    resolved = (2 * all_waves[None, :, None] < point_len[:, None, :]) & in_pair[:, None, :]
    amplitude = jnp.where(resolved, weight_two[None, :, None], 0.0)
    forward_tab = jnp.concatenate([amplitude * cosine, -(amplitude * sine_vals)], 1).astype(
        jnp.bfloat16
    )
    back_tab = jnp.concatenate(
        [jnp.where(resolved, cosine, 0.0), -jnp.where(resolved, sine_vals, 0.0)], 1
    ).astype(jnp.bfloat16)
    forward_tiles = forward_tab.reshape(quarter, 2 * wave_count, tile_count, 128)
    back_tiles = back_tab.reshape(quarter, 2 * wave_count, tile_count, 128)
    tile_start = jnp.arange(tile_count, dtype=jnp.int32)[None, :] * 128
    owner_second = tile_start + 128 > first_len
    boundary = first_len[:, 0] // 128
    is_bound = jnp.arange(tile_count, dtype=jnp.int32)[None, :] == boundary[:, None]
    first_tiles = first_lat.reshape(quarter, tile_count, 128)
    stacked = coeffs.reshape(quarter, 2, 2, wave_count, 2, flat_rows).transpose(0, 1, 2, 4, 3, 5)
    stacked = stacked.reshape(quarter, 2, 2, 2 * wave_count, flat_rows)
    coef_tiles = jnp.where(
        owner_second[:, None, :, None, None],
        stacked[:, :, 1][:, :, None],
        stacked[:, :, 0][:, :, None],
    )
    grid_tiles = jnp.einsum(
        "qatkf,qktp->qaftp", coef_tiles, forward_tiles, preferred_element_type=jnp.float32
    )
    bound_fwd = jnp.take_along_axis(forward_tiles, boundary[:, None, None, None], axis=2)[:, :, 0]
    bound_back = jnp.take_along_axis(back_tiles, boundary[:, None, None, None], axis=2)[:, :, 0]
    edge_grid = jnp.einsum(
        "qakf,qkp->qafp", stacked[:, :, 0], bound_fwd, preferred_element_type=jnp.float32
    )
    use_edge = is_bound[:, :, None] & first_tiles
    grid_tiles = jnp.where(use_edge[:, None, None], edge_grid[:, :, :, None, :], grid_tiles)
    grid_vals = grid_tiles.reshape(quarter, 2, field_stack, layers_on_processor, padded)
    row_cor = planetary_rotation_effect.reshape(quarter, 2, 2)
    point_cor = jnp.where(first_lat[:, None, :], row_cor[:, :, 0:1], row_cor[:, :, 1:2])[
        :, :, None, :
    ]
    products = rate_bundle(
        grid_vals[:, :, 0], grid_vals[:, :, 1], grid_vals[:, :, 2], grid_vals[:, :, 3], point_cor, 2
    )
    products = products.astype(jnp.bfloat16).reshape(quarter, 2, flat_rows, tile_count, 128)
    keep = jnp.where(owner_second[:, :, None], jnp.logical_not(first_tiles), first_tiles)
    main_prods = jnp.where(keep[:, None, None], products, jnp.zeros_like(products))
    per_tile = jnp.einsum(
        "qaftp,qktp->qatkf", main_prods, back_tiles, preferred_element_type=jnp.float32
    )
    bound_prods = jnp.take_along_axis(products, boundary[:, None, None, None, None], axis=3)[
        :, :, :, 0
    ]
    bound_first = jnp.take_along_axis(first_tiles, boundary[:, None, None], axis=1)[:, 0]
    bound_prods = jnp.where(bound_first[:, None, None, :], bound_prods, jnp.zeros_like(bound_prods))
    edge_back = jnp.einsum(
        "qafp,qkp->qakf", bound_prods, bound_back, preferred_element_type=jnp.float32
    )
    owner_mask = owner_second[:, None, :, None, None]
    first_ret = jnp.sum(jnp.where(owner_mask, 0.0, per_tile), axis=2) + edge_back
    second_ret = jnp.sum(jnp.where(owner_mask, per_tile, 0.0), axis=2)
    returned = jnp.stack([first_ret, second_ret], axis=2)
    returned = (returned * row_scale.reshape(quarter, 2, 2)[:, :, :, None, None]).astype(
        jnp.bfloat16
    )
    out_rows = returned.reshape(quarter, 2, 2, 2, wave_count, flat_rows).transpose(0, 1, 2, 4, 3, 5)
    out_rows = out_rows.reshape(per_dev, wave_count * columns)
    gathered_rows = lax.all_to_all(out_rows, "wave", split_axis=1, concat_axis=0, tiled=True)
    inverse = (
        jnp.zeros((total_lat,), jnp.int32)
        .at[send_order]
        .set(jnp.arange(total_lat, dtype=jnp.int32))
    )
    back_fourier = jnp.take(gathered_rows, inverse, axis=0).reshape(
        total_lat, number_of_slots, columns
    )
    tendency = jnp.einsum(
        "lsc,sln->scn", back_fourier, legendre, preferred_element_type=jnp.float32
    )
    tendency = tendency.reshape(number_of_slots, 2, field_stack, layers_on_processor, degree_list)
    tendency = tendency.at[:, :, 2].add(geopot)
    tendency = jnp.where(valid_cols[:, None, None, None, :], tendency, 0.0)
    return tendency.reshape(number_of_slots, columns, degree_list).astype(jnp.bfloat16)


def solution(mesh):
    def body(spec, legendre, layer_depth_share, quad_weight, wave_of_slot):
        slots, cols, span = spec.shape
        layers = layer_depth_share.shape[0]
        n = Sizes(mesh.shape["wave"], mesh.shape["lev"], slots, cols, legendre.shape[1], span, layers)
        step = (lambda *args: fast_body(n, *args)) if n.fits() else general_body
        return step(spec, legendre, layer_depth_share, quad_weight, wave_of_slot)

    in_specs = (P("wave", "lev", None), P("wave", None, None), P("lev"), P(), P("wave"))
    out_specs = P("wave", "lev", None)
    return jax.shard_map(body, mesh=mesh, in_specs=in_specs, out_specs=out_specs, check_vma=False)
```

```python
import math

import numpy as np
import jax
import jax.numpy as jnp
from jax import lax
from jax.experimental import pallas as pl
from jax.experimental.pallas import tpu as pltpu
from jax.sharding import PartitionSpec as P

bf16 = jnp.bfloat16
f32 = jnp.float32
FIELDS = 4
IMAGES = 4
LANES = 128
ROUNDER = 12582912.0
CHUNK = 256
GROUP = 2
PIECES = 2
FLIGHT = 2


def nt(a, b):
    return lax.dot_general(a, b, (((1,), (1,)), ((), ())), preferred_element_type=f32)


def nn(a, b):
    return lax.dot_general(a, b, (((1,), (0,)), ((), ())), preferred_element_type=f32)


def circle_polynomials():
    f = np.cos(np.pi * (np.arange(4000) + 0.5) / 8000) * 0.505
    z = f * f
    out = []
    for values in (np.cos(np.pi * f), np.sin(np.pi * f) / f):
        fit = np.polynomial.chebyshev.Chebyshev.fit(z, math.sqrt(2.0) * values, 4, domain=[0, 0.2551])
        out.append([float(c) for c in fit.convert(kind=np.polynomial.Polynomial).coef])
    return out


COS_POLY, SIN_POLY = circle_polynomials()


def horner(z, coefs):
    acc = z * coefs[-1] + coefs[-2]
    for c in coefs[-3::-1]:
        acc = acc * z + c
    return acc


def cos_sin(count, length, inverse):
    turns = (count * inverse + ROUNDER) - ROUNDER
    f = (count - turns * length) * inverse
    z = f * f
    half_sin = f * horner(z, SIN_POLY)
    return 1.0 - half_sin * half_sin, half_sin * horner(z, COS_POLY)


def image_signs():
    return np.array([[1, 1, 1, 1], [-1, 1, -1, 1], [1, 1, -1, -1], [-1, 1, 1, -1]], np.float32)


class Sizes:
    def __init__(self, n_wave, n_lev, slots, cols, lats, span, layers):
        self.n_wave, self.n_lev, self.slots, self.cols = n_wave, n_lev, slots, cols
        self.lats, self.span, self.layers = lats, span, layers
        self.rows = lats // n_wave // 2
        self.half = self.rows // 2
        self.circles = lats // 2
        self.points = self.circles + 11
        self.width = -(-self.points // CHUNK) * CHUNK
        self.tiles = self.width // LANES
        self.sent = self.rows + 8
        self.keys = 8 * n_wave

    def fits(self):
        return (
            self.slots == 2
            and self.cols == 32
            and self.layers == 4
            and self.n_wave == 8
            and self.n_lev == 4
            and self.rows % 16 == 0
            and self.half % GROUP == 0
            and self.half % 8 == 0
            and self.half * 4 * self.n_wave == self.lats
            and self.span % LANES == 0
            and (self.n_wave * self.rows) % LANES == 0
            and self.tiles <= 8
        )

    def block_starts(self, owner):
        h = self.half
        return (
            (h * owner, self.circles - h * (owner + 1)),
            (self.lats - h * (owner + 1), self.circles + h * owner),
        )


def order_matrix(n):
    out = np.zeros((LANES, LANES), np.float32)
    for parity in range(2):
        for part in range(2):
            for hemi in range(2):
                for field in range(FIELDS):
                    for layer in range(n.layers):
                        row = hemi * 64 + parity * 32 + part * 16 + field * 4 + layer
                        lane = (parity * 2 + part) * 32 + field * 8 + hemi * 4 + layer
                        out[row, lane] = 1.0
    return out


def live_spec(n, spec, wave):
    degree = lax.broadcasted_iota(jnp.int32, (n.cols, n.span), 1)
    live = degree < n.span - wave
    return jnp.where(live, spec.astype(f32), 0.0), live


def layer_sums(n, masked, share_ref):
    row = lax.broadcasted_iota(jnp.int32, (n.cols, n.span), 0)
    layer = row % n.layers
    weight = jnp.where(
        layer < 2,
        jnp.where(layer == 0, share_ref[0], share_ref[1]),
        jnp.where(layer == 2, share_ref[2], share_ref[3]),
    )
    warm = (row // n.layers) % FIELDS == FIELDS - 1
    y = jnp.where(warm, masked * weight, 0.0)
    y = y + pltpu.roll(y, n.cols - 1, 0)
    return y + pltpu.roll(y, n.cols - 2, 0)


def fetch(pairs, sems):
    copies = [pltpu.make_async_copy(src, dst, sems.at[k]) for k, (src, dst) in enumerate(pairs)]
    for copy in copies:
        copy.start()
    return copies


def forward_kernel(n, wave_hbm, share_hbm, spec_hbm, leg_hbm, out_hbm, total_hbm, leg, high_hbm, wave_ref, share_ref, spec_ref, total_ref, high_ref, acc, sems, leg_sems, done_sems, out_ref, out_sems):
    small = fetch(((wave_hbm, wave_ref), (share_hbm, share_ref), (spec_hbm, spec_ref)), sems)
    size = n.circles // PIECES
    big = [
        [
            pltpu.make_async_copy(leg_hbm.at[s, pl.ds(k * size, size), :], leg.at[s, pl.ds(k * size, size), :], leg_sems.at[s, k])
            for s in range(2)
        ]
        for k in range(2 * PIECES)
    ]
    for pair in big[:FLIGHT]:
        for copy in pair:
            copy.start()
    for copy in small:
        copy.wait()
    row = lax.broadcasted_iota(jnp.int32, (n.cols, n.span), 0)
    target = (row // n.layers) % FIELDS == 2
    tables = [[], []]
    for s in range(2):
        masked, live = live_spec(n, spec_ref[s], wave_ref[s])
        sums = layer_sums(n, masked, share_ref)
        for part in range(2):
            total_ref[2 * s + part : 2 * s + part + 1, :] = sums[part * 16 + 12 : part * 16 + 13, :]
        high_ref[s] = jnp.where(target, pltpu.roll(sums, n.cols - n.layers, 0), 0.0)
        leg[s, n.lats : n.lats + 8, :] = jnp.where(live[:8], 1.0, 0.0).astype(bf16)
        leg[s, n.lats + 8 : n.lats + 16, :] = jnp.full((8, n.span), (1 - wave_ref[s] % 2).astype(f32)).astype(bf16)
        scaled = masked * jnp.where(wave_ref[s] == 0, 1.0, 2.0)
        none = jnp.zeros_like(scaled[:16])
        for hemi in range(2):
            rows = []
            for parity in range(2):
                mine = wave_ref[s] % 2 == parity
                for part in range(2):
                    chunk = jnp.where(mine, scaled[part * 16 : part * 16 + 16], 0.0)
                    rows += [chunk, none] if hemi == 0 else [none, chunk]
            tables[hemi].append(jnp.concatenate(rows, 0).astype(bf16))
    tables = [jnp.concatenate(pair, 1) for pair in tables]
    even = jnp.where(wave_ref[0] % 2 == 0, wave_ref[0], wave_ref[1])
    lane = lax.broadcasted_iota(jnp.int32, (8, LANES), 1)
    tag = jnp.where(lane < LANES // 2, even // 16, even % 16).astype(f32).astype(bf16)
    for owner in range(n.n_wave):
        out_ref[owner, n.rows : n.sent, :] = tag

    def strip(start, count):
        return out_ref.at[:, pl.ds(start, count), :], out_hbm.at[:, pl.ds(start, count), :]

    leaving = fetch(((total_ref, total_hbm), (high_ref, high_hbm), strip(n.rows, 8)), done_sems)
    for k in range(2 * PIECES):
        for copy in big[k]:
            copy.wait()
        if k + FLIGHT < 2 * PIECES:
            for copy in big[k + FLIGHT]:
                copy.start()
        rows = slice(k * size, (k + 1) * size)
        both = jnp.concatenate([leg[0, rows, :], leg[1, rows, :]], 1)
        acc[rows, :] = nt(both, tables[k // PIECES])
        if k >= PIECES and (k + 1) % (PIECES // 2) == 0:
            b = 3 - (k + 1) // (PIECES // 2) + 1
            for owner in range(n.n_wave):
                starts = n.block_starts(owner)
                block = acc[starts[0][b] : starts[0][b] + n.half, :] + acc[starts[1][b] : starts[1][b] + n.half, :]
                out_ref[owner, b * n.half : (b + 1) * n.half, :] = block.astype(bf16)
            copy = pltpu.make_async_copy(*strip(b * n.half, n.half), out_sems.at[b])
            copy.start()
            leaving.append(copy)
    for copy in leaving:
        copy.wait()


def grid_kernel(n, got_ref, sign_ref, near_ref, quad_hbm, total_hbm, out_hbm, pair_hbm, keep_hbm, spread, table_a, table_b, coef_a, coef_b, rows, out, total_ref, pair_ref, keep_ref, quad_ref, out_sem, in_sems, side_sems, inv_ref, cor_ref):
    arriving = fetch(((quad_hbm, quad_ref), (total_hbm, total_ref)), in_sems)
    device = lax.axis_index("wave")
    first_circle = device * n.half
    top = n.span - 1
    lane = lax.broadcasted_iota(jnp.int32, (8, LANES), 1)
    lane_f = lane.astype(f32)
    north = (lane // 4) % 2 == 0
    sent_lane = lax.broadcasted_iota(jnp.int32, (LANES, LANES), 0)
    to = lax.broadcasted_iota(jnp.int32, (LANES, LANES), 1)
    source = (to // 4 % 2) * 16 + (to // 8 % FIELDS) * 4 + to % 4
    for p in range(4):
        pick = jnp.where(sent_lane == source + p * 32, sign_ref[p : p + 1, :], 0.0).astype(bf16)
        wide = nn(got_ref[...], pick)
        for src in range(n.n_wave):
            for r in range(0, n.rows, 8):
                spread[p, pl.ds(r * n.n_wave + src, 8, stride=n.n_wave), :] = wide[src * n.sent + r : src * n.sent + r + 8]
    raw = got_rows_f32(n, got_ref)
    tag = jnp.where(lane < LANES // 2, raw * 16.0, raw)
    even_m = tag + pltpu.roll(tag, LANES // 2, 1)
    odd_m = float(top) - even_m
    even_2 = 2.0 * even_m
    odd_2 = 2.0 * odd_m
    for k in range(2):
        step = lax.broadcasted_iota(jnp.int32, (n.half, LANES), 0)
        circle = first_circle + step if k == 0 else n.circles - 1 - first_circle - step
        inv_ref[k] = 1.0 / (20 + 4 * circle).astype(f32)
        whole = jnp.full((n.half, LANES), 4.0 * n.lats, f32)
        cosine, _ = cos_sin((2 * circle + 1).astype(f32), whole, 1.0 / (4 * n.lats))
        cor_ref[k] = 2.0 * cosine
    tile_point = (lax.broadcasted_iota(jnp.int32, (8, LANES), 0) * LANES + lane).astype(f32)

    def sizes(i):
        short = first_circle + i
        return short, n.circles - 1 - short

    def build(i, u, table):
        short, long = sizes(i)
        cut = (short + 6).astype(f32)
        len_s = (20 + 4 * short).astype(f32)
        len_l = (20 + 4 * long).astype(f32)
        inv_s = inv_ref[0, pl.ds(i, 1), :]
        inv_l = inv_ref[1, pl.ds(i, 1), :]

        def places(point):
            own = point < cut
            return jnp.where(own, point, point - cut), jnp.where(own, len_s, len_l), jnp.where(own, inv_s, inv_l)

        j, length, inverse = places(tile_point)
        top_c, top_s = cos_sin(j * float(top), length, inverse)
        for t in range(n.tiles):
            j, length, inverse = places(lane_f + float(t * LANES))
            c, s = cos_sin(even_m * j, length, inverse)
            tc = jnp.broadcast_to(top_c[t : t + 1, :], (8, LANES))
            ts = jnp.broadcast_to(top_s[t : t + 1, :], (8, LANES))
            span = slice(t * LANES, (t + 1) * LANES)
            table[u, 0:8, span] = c
            table[u, 8:16, span] = s
            table[u, 16:24, span] = tc * c + ts * s
            table[u, 24:32, span] = ts * c - tc * s

    def gather(i, u, coef):
        short, long = sizes(i)
        parts = []
        for circle, row_n, row_s in (
            (short, i, n.half - 1 - i),
            (long, n.rows - 1 - i, n.half + i),
        ):
            length = (20 + 4 * circle).astype(f32)
            for p in range(4):
                up = spread[p, pl.ds(row_n * 8, 8), :]
                down = spread[p, pl.ds(row_s * 8, 8), :]
                seen = (odd_2 if p > 1 else even_2) < length
                parts.append(jnp.where(seen, jnp.where(north, up, down), 0.0))
        coef[u] = jnp.transpose(jnp.concatenate(parts, 0))

    south = lax.broadcasted_iota(jnp.int32, (8, LANES), 0) // 4
    lane_b = lax.broadcasted_iota(jnp.int32, (16, LANES), 1).astype(f32).astype(bf16)
    signs = [sign_ref[p : p + 1, :] for p in range(4)]
    group = lane // 32
    kinetic = jnp.where((lane // 8) % FIELDS == 2, 0.5, 1.0)

    def weights(t, cut):
        edge_at = jnp.clip(cut - t * LANES, -4, LANES + 4).astype(f32) - 0.5
        x = jnp.full((16, LANES), edge_at, f32).astype(bf16) - lane_b
        share = jnp.minimum(jnp.abs(x), 1.0)
        own = jnp.minimum(jnp.maximum(x + 0.5, 0.0), 1.0)
        if t == 0 or (t + 1) * LANES >= n.points:
            point = lax.broadcasted_iota(jnp.int32, (16, LANES), 1) + t * LANES
            ends = (point == 0) | (point == n.points - 1)
            share = share * jnp.where(ends, 0.5, jnp.where(point < n.points, 1.0, 0.0)).astype(bf16)
        own_share = own * share
        return own, 1.0 - own, own_share, share - own_share

    def transform(i, u, table, coef):
        short, long = sizes(i)
        cut = short + 6
        left = coef[u].astype(bf16)
        cor_s = cor_ref[0, pl.ds(i, 1), :]
        cor_l = cor_ref[1, pl.ds(i, 1), :]
        total = None
        for c in range(n.width // CHUNK):
            ahead, behind, spins = [], [], []
            for t in range(c * CHUNK // LANES, (c + 1) * CHUNK // LANES):
                tab = table[u, :, t * LANES : (t + 1) * LANES].astype(bf16)
                own, rest, own_share, rest_share = weights(t, cut)
                if c * CHUNK >= n.circles // 2 + 6:
                    ahead.append(jnp.concatenate([jnp.zeros_like(tab), tab], 0))
                    share = own_share + rest_share
                    behind.append(jnp.concatenate([tab[:16] * share, tab[16:] * share], 0))
                    spins.append(jnp.where(south == 0, cor_l, -cor_l))
                    continue
                ahead.append(jnp.concatenate([tab[:16] * own, tab[16:] * own, tab[:16] * rest, tab[16:] * rest], 0))
                behind.append(
                    jnp.concatenate(
                        [tab[:16] * own_share, tab[16:] * own_share, tab[:16] * rest_share, tab[16:] * rest_share], 0
                    )
                )
                spin = jnp.where(lane < cut - t * LANES, cor_s, cor_l)
                spins.append(jnp.where(south == 0, spin, -spin))
            grid = nn(left, jnp.concatenate(ahead, 1)).reshape(IMAGES, FIELDS, 8, CHUNK)
            x, y, curl, warm = grid[:, 0], grid[:, 1], grid[:, 2], grid[:, 3]
            absolute = curl + jnp.concatenate(spins, 1)
            prods = jnp.stack([absolute * x, absolute * y, x * x + y * y, x * warm], 1)
            piece = nt(jnp.concatenate(behind, 1), prods.reshape(LANES, CHUNK).astype(bf16))
            if piece.shape[0] < n.keys:
                piece = jnp.concatenate([jnp.zeros_like(piece), piece], 0)
            total = piece if total is None else total + piece
        results = []
        for k, circle in enumerate((short, long)):
            length = (20 + 4 * circle).astype(f32)
            folded = None
            for p in range(4):
                y = total[(4 * k + p) * 8 : (4 * k + p + 1) * 8] * signs[p]
                y = y + pltpu.roll(y, 64, 1)
                y = y + pltpu.roll(y, 32, 1)
                y = jnp.where((odd_2 if p > 1 else even_2) < length, y, 0.0)
                folded = y if folded is None else jnp.where(group == p, y, folded)
            weight = jnp.where(north, quad_ref[circle], quad_ref[n.lats - 1 - circle])
            results.append(folded * (weight * (inv_ref[k, pl.ds(i, 1), :] * kinetic)))
        return results

    turns = [i for k in range(n.half // 2) for i in (k, n.half - 1 - k)]
    groups = [turns[k : k + GROUP] for k in range(0, n.half, GROUP)]

    def ready(members, table, coef):
        for u, i in enumerate(members):
            build(i, u, table)
            gather(i, u, coef)

    def work(members, table, coef):
        for u in range(0, GROUP, 2):
            i, other = members[u : u + 2]
            short_i, long_i = transform(i, u, table, coef)
            short_o, long_o = transform(other, u + 1, table, coef)
            for at, up, down in (
                (i, short_i, short_o),
                (other, short_o, short_i),
                (n.half + i, long_o, long_i),
                (n.half + other, long_i, long_o),
            ):
                rows[pl.ds(at, 8, stride=n.rows), :] = jnp.where(north, up, down)

    ready(groups[0], table_a, coef_a)
    for copy in arriving:
        copy.wait()
    pair_ref[...] = total_ref[...] + near_ref[...]
    keep_ref[...] = jnp.where(lax.axis_index("lev") % 2 == 0, near_ref[...], 0.0)
    leaving = fetch(((pair_ref, pair_hbm), (keep_ref, keep_hbm)), side_sems)
    buffers = ((table_a, coef_a), (table_b, coef_b))
    for k, members in enumerate(groups):
        if k + 1 < len(groups):
            ready(groups[k + 1], *buffers[(k + 1) % 2])
        work(members, *buffers[k % 2])

    out[...] = rows[...].astype(bf16)
    copy = pltpu.make_async_copy(out, out_hbm, out_sem)
    copy.start()
    for side in leaving:
        side.wait()
    copy.wait()


def got_rows_f32(n, got_ref):
    pieces = [got_ref[src * n.sent + n.rows : src * n.sent + n.rows + 8, :].astype(f32)[:1] for src in range(n.n_wave)]
    return jnp.concatenate(pieces, 0)


def back_kernel(n, far_hbm, keep_hbm, high_hbm, back_ref, order_ref, leg, out_ref, turn, far_ref, keep_ref, high_ref, sems):
    arriving = fetch(((far_hbm, far_ref), (keep_hbm, keep_ref), (high_hbm, high_ref)), sems)
    for owner in range(n.n_wave):
        starts = n.block_starts(owner)
        for b in range(2):
            block = back_ref[owner * n.rows + b * n.half : owner * n.rows + (b + 1) * n.half, :]
            for hemi in range(2):
                at = starts[hemi][b] - hemi * n.circles
                turn[hemi, at : at + n.half, :] = block
    turned = [nt(order_ref[hemi * 64 : hemi * 64 + 64, :], turn[hemi]) for hemi in range(2)]
    row = lax.broadcasted_iota(jnp.int32, (n.cols, n.span), 0)
    target = (row // n.layers) % FIELDS == 2
    sums = []
    for s in range(2):
        even = leg[s, n.lats + 8 : n.lats + 16, :].astype(f32)[:1] > 0.5
        for hemi in range(2):
            mine = jnp.where(even, turned[hemi][:32], turned[hemi][32:]).astype(bf16)
            piece = nn(mine, leg[s, hemi * n.circles : (hemi + 1) * n.circles, :])
            sums.append(piece if hemi == 0 else sums.pop() + piece)
    for copy in arriving:
        copy.wait()
    deeper = keep_ref[...] + jnp.where(lax.axis_index("lev") < n.n_lev // 2, far_ref[...], 0.0)
    for s in range(2):
        live = leg[s, n.lats : n.lats + 8, :].astype(f32)[:1] > 0.5
        low = jnp.where(row < 16, deeper[2 * s : 2 * s + 1], deeper[2 * s + 1 : 2 * s + 2])
        tendency = sums[s] + high_ref[s] + jnp.where(target, low, 0.0)
        out_ref[s] = jnp.where(live, tendency, 0.0).astype(bf16)


def stay(*arrays, space=pltpu.HBM):
    return [pltpu.with_memory_space_constraint(x, space) for x in arrays]


def kernel_params():
    return pltpu.CompilerParams(
        vmem_limit_bytes=24 * 1024 * 1024
    )


def smem():
    return pl.BlockSpec(memory_space=pltpu.SMEM)


def vmem():
    return pl.BlockSpec(memory_space=pltpu.VMEM)


def hbm():
    return pl.BlockSpec(memory_space=pltpu.HBM)


def grid_call(n, got, quad_weight, totals, near):
    all_rows = n.n_wave * n.rows
    signs = np.zeros((8, LANES), np.float32)
    signs[:4] = np.repeat(image_signs(), LANES // IMAGES, axis=1)
    table = pltpu.VMEM((GROUP, n.keys // 2, n.width), f32)
    coef = pltpu.VMEM((GROUP, LANES, n.keys), f32)
    return pl.pallas_call(
        lambda *refs: grid_kernel(n, *refs),
        out_shape=(pltpu.HBM((all_rows, LANES), bf16), pltpu.HBM(totals.shape, f32), pltpu.HBM(totals.shape, f32)),
        in_specs=[vmem()] * 3 + [hbm()] * 2,
        out_specs=(hbm(),) * 3,
        scratch_shapes=[
            pltpu.VMEM((4, n.n_wave * n.rows, LANES), f32),
            table,
            table,
            coef,
            coef,
            pltpu.VMEM((all_rows, LANES), f32),
            pltpu.VMEM((all_rows, LANES), bf16),
            pltpu.VMEM(totals.shape, f32),
            pltpu.VMEM(totals.shape, f32),
            pltpu.VMEM(totals.shape, f32),
            pltpu.SMEM((n.lats,), f32),
            pltpu.SemaphoreType.DMA,
            pltpu.SemaphoreType.DMA((2,)),
            pltpu.SemaphoreType.DMA((2,)),
            pltpu.VMEM((2, n.half, LANES), f32),
            pltpu.VMEM((2, n.half, LANES), f32),
        ],
        compiler_params=kernel_params(),
        name="grid_stage",
    )(
        got,
        jnp.asarray(signs),
        near,
        *stay(quad_weight, totals),
    )


def fast_body(n, spec, legendre, layer_depth_share, quad_weight, wave_of_slot):
    params = kernel_params()
    all_rows = n.n_wave * n.rows
    dma = pltpu.SemaphoreType.DMA
    held_shape = (2, n.lats + 16, n.span)
    high_shape = (2, n.cols, n.span)
    total_shape = (4, n.span)
    sent, totals, held, high = pl.pallas_call(
        lambda *refs: forward_kernel(n, *refs),
        out_shape=(
            pltpu.HBM((n.n_wave, n.sent, LANES), bf16),
            pltpu.HBM(total_shape, f32),
            pltpu.VMEM(held_shape, bf16),
            pltpu.HBM(high_shape, f32),
        ),
        in_specs=[hbm()] * 4,
        out_specs=(hbm(), hbm(), vmem(), hbm()),
        scratch_shapes=[
            pltpu.SMEM((2,), jnp.int32),
            pltpu.SMEM((n.layers,), f32),
            pltpu.VMEM(spec.shape, bf16),
            pltpu.VMEM(total_shape, f32),
            pltpu.VMEM(high_shape, f32),
            pltpu.VMEM((n.lats, LANES), f32),
            dma((3,)),
            dma((2, 2 * PIECES)),
            dma((3,)),
            pltpu.VMEM((n.n_wave, n.sent, LANES), bf16),
            dma((2,)),
        ],
        compiler_params=params,
        name="legendre_forward",
    )(*stay(wave_of_slot, layer_depth_share, spec, legendre))
    near = lax.ppermute(totals, "lev", [(i, i ^ 1) for i in range(n.n_lev)])
    got = lax.all_to_all(sent, "wave", split_axis=0, concat_axis=0, tiled=True)
    out, pair, keep = grid_call(n, got.reshape(n.n_wave * n.sent, LANES), quad_weight, totals, near)
    far = lax.ppermute(pair, "lev", [(i, i ^ 2) for i in range(n.n_lev)])
    back = lax.all_to_all(
        out.reshape(n.n_wave, n.rows, LANES), "wave", split_axis=0, concat_axis=0, tiled=True
    )
    return pl.pallas_call(
        lambda *refs: back_kernel(n, *refs),
        out_shape=jax.ShapeDtypeStruct(spec.shape, bf16),
        in_specs=[hbm()] * 3 + [vmem()] * 3,
        out_specs=vmem(),
        scratch_shapes=[
            pltpu.VMEM((2, n.circles, LANES), bf16),
            pltpu.VMEM(total_shape, f32),
            pltpu.VMEM(total_shape, f32),
            pltpu.VMEM(high_shape, f32),
            dma((3,)),
        ],
        compiler_params=params,
        name="legendre_back",
    )(
        *stay(far, keep, high),
        back.reshape(all_rows, LANES),
        jnp.asarray(order_matrix(n), bf16),
        *stay(held, space=pltpu.VMEM),
    )


full_turn = 2.0 * math.pi


def carried_in(part, axis, combine, identity):
    count = lax.axis_size(axis)
    place = lax.axis_index(axis)
    ahead = count - 1 - place
    gathered = lax.all_gather(part, axis)
    state = jnp.zeros_like(part) + jnp.asarray(identity, part.dtype)

    def one(hop, state):
        source = count - 1 - hop
        return combine(state, lax.dynamic_index_in_dim(gathered, source, 0, False))

    return lax.fori_loop(0, ahead, one, state)


def rate_bundle(
    eastward_velocity,
    northward_velocity,
    local_curl_spin,
    thermal_state,
    planetary_rotation_effect,
    processor_dimension,
):
    absolute = local_curl_spin + planetary_rotation_effect
    return jnp.stack(
        [
            absolute * eastward_velocity,
            absolute * northward_velocity,
            0.5 * (eastward_velocity * eastward_velocity + northward_velocity * northward_velocity),
            eastward_velocity * thermal_state,
        ],
        axis=processor_dimension,
    )


def row_latitudes(device, per_dev, total_lat):
    row_ids = jnp.arange(per_dev, dtype=jnp.int32)
    quarter = per_dev // 4
    block_ids = row_ids // 4
    hemisphere = row_ids // 2 % 2
    member = row_ids % 2
    first_dist = device * quarter + block_ids
    pole_dist = jnp.where(member == 0, first_dist, total_lat // 2 - 1 - first_dist)
    return jnp.where(hemisphere == 0, pole_dist, total_lat - 1 - pole_dist)


def add_terms(earlier, later):
    return earlier + later


def general_body(spec, legendre, layer_depth_share, quad_weight, wave_of_slot):
    number_of_slots, columns, degree_list = spec.shape
    total_lat = legendre.shape[1]
    groups = lax.axis_size("wave")
    device = lax.axis_index("wave")
    per_dev = total_lat // groups
    layers_on_processor = layer_depth_share.shape[0]
    field_stack = columns // (2 * layers_on_processor)
    flat_rows = field_stack * layers_on_processor
    max_points = 20 + 4 * (total_lat // 2 - 1)
    all_waves = lax.all_gather(wave_of_slot, "wave", axis=0, tiled=True)
    wave_count = all_waves.shape[0]
    weight_two = jnp.where(all_waves == 0, 1.0, 2.0).astype(jnp.float32)
    degree_index = jnp.arange(degree_list, dtype=jnp.int32)
    valid_cols = degree_index[None, :] < (degree_list - wave_of_slot)[:, None]
    screened_entries = jnp.where(valid_cols[:, None, :], spec, jnp.zeros_like(spec))
    thermal_state = screened_entries.reshape(
        number_of_slots, 2, field_stack, layers_on_processor, degree_list
    )[:, :, 3].astype(jnp.float32)
    scaled_entries = thermal_state * layer_depth_share[None, None, :, None]
    below_sum = jnp.flip(jnp.cumsum(jnp.flip(scaled_entries, 2), 2), 2)
    deeper = carried_in(
        below_sum[:, :, 0],
        "lev",
        add_terms,
        jnp.zeros((number_of_slots, 2, degree_list), jnp.float32),
    )
    geopot = below_sum + deeper[:, :, None, :]
    fourier = jnp.einsum(
        "sln,scn->lsc", legendre, screened_entries, preferred_element_type=jnp.float32
    ).astype(jnp.bfloat16)
    send_order = row_latitudes(
        jnp.arange(groups, dtype=jnp.int32)[:, None], per_dev, total_lat
    ).reshape(-1)
    send_rows = jnp.take(fourier, send_order, axis=0).reshape(total_lat, number_of_slots * columns)
    received = lax.all_to_all(send_rows, "wave", split_axis=0, concat_axis=1, tiled=True)
    coeffs = received.reshape(per_dev, wave_count, 2, flat_rows)
    latitudes = row_latitudes(device, per_dev, total_lat)
    lengths = 20 + 4 * jnp.minimum(latitudes, total_lat - 1 - latitudes)
    planetary_rotation_effect = 2.0 * jnp.cos(
        (latitudes.astype(jnp.float32) + 0.5) * (math.pi / total_lat)
    )
    row_scale = quad_weight[latitudes] / lengths.astype(jnp.float32)
    quarter = per_dev // 4
    pair_points = max_points + 20
    tile_count = -(-pair_points // 128)
    padded = tile_count * 128
    pair_len = lengths.reshape(quarter, 2, 2)[:, 0, :]
    first_len = pair_len[:, 0:1]
    second_len = pair_len[:, 1:2]
    points = jnp.arange(padded, dtype=jnp.int32)[None, :]
    first_lat = points < first_len
    in_pair = points < pair_points
    local_idx = jnp.where(first_lat, points, points - first_len)
    point_len = jnp.where(first_lat, first_len, second_len)
    phase_int = all_waves[None, :, None] * local_idx[:, None, :] % point_len[:, None, :]
    angles = phase_int.astype(jnp.float32) * full_turn / point_len.astype(jnp.float32)[:, None, :]
    cosine = jnp.cos(angles)
    sine_vals = jnp.sin(angles)
    resolved = (2 * all_waves[None, :, None] < point_len[:, None, :]) & in_pair[:, None, :]
    amplitude = jnp.where(resolved, weight_two[None, :, None], 0.0)
    forward_tab = jnp.concatenate([amplitude * cosine, -(amplitude * sine_vals)], 1).astype(
        jnp.bfloat16
    )
    back_tab = jnp.concatenate(
        [jnp.where(resolved, cosine, 0.0), -jnp.where(resolved, sine_vals, 0.0)], 1
    ).astype(jnp.bfloat16)
    forward_tiles = forward_tab.reshape(quarter, 2 * wave_count, tile_count, 128)
    back_tiles = back_tab.reshape(quarter, 2 * wave_count, tile_count, 128)
    tile_start = jnp.arange(tile_count, dtype=jnp.int32)[None, :] * 128
    owner_second = tile_start + 128 > first_len
    boundary = first_len[:, 0] // 128
    is_bound = jnp.arange(tile_count, dtype=jnp.int32)[None, :] == boundary[:, None]
    first_tiles = first_lat.reshape(quarter, tile_count, 128)
    stacked = coeffs.reshape(quarter, 2, 2, wave_count, 2, flat_rows).transpose(0, 1, 2, 4, 3, 5)
    stacked = stacked.reshape(quarter, 2, 2, 2 * wave_count, flat_rows)
    coef_tiles = jnp.where(
        owner_second[:, None, :, None, None],
        stacked[:, :, 1][:, :, None],
        stacked[:, :, 0][:, :, None],
    )
    grid_tiles = jnp.einsum(
        "qatkf,qktp->qaftp", coef_tiles, forward_tiles, preferred_element_type=jnp.float32
    )
    bound_fwd = jnp.take_along_axis(forward_tiles, boundary[:, None, None, None], axis=2)[:, :, 0]
    bound_back = jnp.take_along_axis(back_tiles, boundary[:, None, None, None], axis=2)[:, :, 0]
    edge_grid = jnp.einsum(
        "qakf,qkp->qafp", stacked[:, :, 0], bound_fwd, preferred_element_type=jnp.float32
    )
    use_edge = is_bound[:, :, None] & first_tiles
    grid_tiles = jnp.where(use_edge[:, None, None], edge_grid[:, :, :, None, :], grid_tiles)
    grid_vals = grid_tiles.reshape(quarter, 2, field_stack, layers_on_processor, padded)
    row_cor = planetary_rotation_effect.reshape(quarter, 2, 2)
    point_cor = jnp.where(first_lat[:, None, :], row_cor[:, :, 0:1], row_cor[:, :, 1:2])[
        :, :, None, :
    ]
    products = rate_bundle(
        grid_vals[:, :, 0], grid_vals[:, :, 1], grid_vals[:, :, 2], grid_vals[:, :, 3], point_cor, 2
    )
    products = products.astype(jnp.bfloat16).reshape(quarter, 2, flat_rows, tile_count, 128)
    keep = jnp.where(owner_second[:, :, None], jnp.logical_not(first_tiles), first_tiles)
    main_prods = jnp.where(keep[:, None, None], products, jnp.zeros_like(products))
    per_tile = jnp.einsum(
        "qaftp,qktp->qatkf", main_prods, back_tiles, preferred_element_type=jnp.float32
    )
    bound_prods = jnp.take_along_axis(products, boundary[:, None, None, None, None], axis=3)[
        :, :, :, 0
    ]
    bound_first = jnp.take_along_axis(first_tiles, boundary[:, None, None], axis=1)[:, 0]
    bound_prods = jnp.where(bound_first[:, None, None, :], bound_prods, jnp.zeros_like(bound_prods))
    edge_back = jnp.einsum(
        "qafp,qkp->qakf", bound_prods, bound_back, preferred_element_type=jnp.float32
    )
    owner_mask = owner_second[:, None, :, None, None]
    first_ret = jnp.sum(jnp.where(owner_mask, 0.0, per_tile), axis=2) + edge_back
    second_ret = jnp.sum(jnp.where(owner_mask, per_tile, 0.0), axis=2)
    returned = jnp.stack([first_ret, second_ret], axis=2)
    returned = (returned * row_scale.reshape(quarter, 2, 2)[:, :, :, None, None]).astype(
        jnp.bfloat16
    )
    out_rows = returned.reshape(quarter, 2, 2, 2, wave_count, flat_rows).transpose(0, 1, 2, 4, 3, 5)
    out_rows = out_rows.reshape(per_dev, wave_count * columns)
    gathered_rows = lax.all_to_all(out_rows, "wave", split_axis=1, concat_axis=0, tiled=True)
    inverse = (
        jnp.zeros((total_lat,), jnp.int32)
        .at[send_order]
        .set(jnp.arange(total_lat, dtype=jnp.int32))
    )
    back_fourier = jnp.take(gathered_rows, inverse, axis=0).reshape(
        total_lat, number_of_slots, columns
    )
    tendency = jnp.einsum(
        "lsc,sln->scn", back_fourier, legendre, preferred_element_type=jnp.float32
    )
    tendency = tendency.reshape(number_of_slots, 2, field_stack, layers_on_processor, degree_list)
    tendency = tendency.at[:, :, 2].add(geopot)
    tendency = jnp.where(valid_cols[:, None, None, None, :], tendency, 0.0)
    return tendency.reshape(number_of_slots, columns, degree_list).astype(jnp.bfloat16)


def solution(mesh):
    def body(spec, legendre, layer_depth_share, quad_weight, wave_of_slot):
        slots, cols, span = spec.shape
        layers = layer_depth_share.shape[0]
        n = Sizes(mesh.shape["wave"], mesh.shape["lev"], slots, cols, legendre.shape[1], span, layers)
        step = (lambda *args: fast_body(n, *args)) if n.fits() else general_body
        return step(spec, legendre, layer_depth_share, quad_weight, wave_of_slot)

    in_specs = (P("wave", "lev", None), P("wave", None, None), P("lev"), P(), P("wave"))
    out_specs = P("wave", "lev", None)
    return jax.shard_map(body, mesh=mesh, in_specs=in_specs, out_specs=out_specs, check_vma=False)
```

```python
import math

import numpy as np
import jax
import jax.numpy as jnp
from jax import lax
from jax.experimental import pallas as pl
from jax.experimental.pallas import tpu as pltpu
from jax.sharding import PartitionSpec as P

bf16 = jnp.bfloat16
f32 = jnp.float32
FIELDS = 4
IMAGES = 4
LANES = 128
ROUNDER = 12582912.0
CHUNK = 256
GROUP = 2
PIECES = 2
FLIGHT = 2


def nt(a, b):
    return lax.dot_general(a, b, (((1,), (1,)), ((), ())), preferred_element_type=f32)


def nn(a, b):
    return lax.dot_general(a, b, (((1,), (0,)), ((), ())), preferred_element_type=f32)


def circle_polynomials():
    f = np.cos(np.pi * (np.arange(4000) + 0.5) / 8000) * 0.505
    z = f * f
    out = []
    for values in (np.cos(np.pi * f), np.sin(np.pi * f) / f):
        fit = np.polynomial.chebyshev.Chebyshev.fit(z, math.sqrt(2.0) * values, 4, domain=[0, 0.2551])
        out.append([float(c) for c in fit.convert(kind=np.polynomial.Polynomial).coef])
    return out


COS_POLY, SIN_POLY = circle_polynomials()


def horner(z, coefs):
    acc = z * coefs[-1] + coefs[-2]
    for c in coefs[-3::-1]:
        acc = acc * z + c
    return acc


def cos_sin(count, length, inverse):
    turns = (count * inverse + ROUNDER) - ROUNDER
    f = (count - turns * length) * inverse
    z = f * f
    half_sin = f * horner(z, SIN_POLY)
    return 1.0 - half_sin * half_sin, half_sin * horner(z, COS_POLY)


def image_signs():
    return np.array([[1, 1, 1, 1], [-1, 1, -1, 1], [1, 1, -1, -1], [-1, 1, 1, -1]], np.float32)


class Sizes:
    def __init__(self, n_wave, n_lev, slots, cols, lats, span, layers):
        self.n_wave, self.n_lev, self.slots, self.cols = n_wave, n_lev, slots, cols
        self.lats, self.span, self.layers = lats, span, layers
        self.rows = lats // n_wave // 2
        self.half = self.rows // 2
        self.circles = lats // 2
        self.points = self.circles + 11
        self.width = -(-self.points // CHUNK) * CHUNK
        self.tiles = self.width // LANES
        self.sent = self.rows + 8
        self.keys = 8 * n_wave

    def fits(self):
        return (
            self.slots == 2
            and self.cols == 32
            and self.layers == 4
            and self.n_wave == 8
            and self.n_lev == 4
            and self.rows % 16 == 0
            and self.half % GROUP == 0
            and self.half % 8 == 0
            and self.half * 4 * self.n_wave == self.lats
            and self.span % LANES == 0
            and (self.n_wave * self.rows) % LANES == 0
            and self.tiles <= 8
        )

    def block_starts(self, owner):
        h = self.half
        return (
            (h * owner, self.circles - h * (owner + 1)),
            (self.lats - h * (owner + 1), self.circles + h * owner),
        )


def order_matrix(n):
    out = np.zeros((LANES, LANES), np.float32)
    for parity in range(2):
        for part in range(2):
            for hemi in range(2):
                for field in range(FIELDS):
                    for layer in range(n.layers):
                        row = hemi * 64 + parity * 32 + part * 16 + field * 4 + layer
                        lane = (parity * 2 + part) * 32 + field * 8 + hemi * 4 + layer
                        out[row, lane] = 1.0
    return out


def live_spec(n, spec, wave):
    degree = lax.broadcasted_iota(jnp.int32, (n.cols, n.span), 1)
    live = degree < n.span - wave
    return jnp.where(live, spec.astype(f32), 0.0), live


def layer_sums(n, masked, share_ref):
    row = lax.broadcasted_iota(jnp.int32, (n.cols, n.span), 0)
    layer = row % n.layers
    weight = jnp.where(
        layer < 2,
        jnp.where(layer == 0, share_ref[0], share_ref[1]),
        jnp.where(layer == 2, share_ref[2], share_ref[3]),
    )
    warm = (row // n.layers) % FIELDS == FIELDS - 1
    y = jnp.where(warm, masked * weight, 0.0)
    y = y + pltpu.roll(y, n.cols - 1, 0)
    return y + pltpu.roll(y, n.cols - 2, 0)


def fetch(pairs, sems):
    copies = [pltpu.make_async_copy(src, dst, sems.at[k]) for k, (src, dst) in enumerate(pairs)]
    for copy in copies:
        copy.start()
    return copies


def forward_kernel(n, wave_hbm, share_hbm, spec_hbm, leg_hbm, out_hbm, total_hbm, leg, high_hbm, wave_ref, share_ref, spec_ref, total_ref, high_ref, acc, sems, leg_sems, done_sems, out_ref, out_sems):
    small = fetch(((wave_hbm, wave_ref), (share_hbm, share_ref), (spec_hbm, spec_ref)), sems)
    size = n.circles // PIECES
    big = [
        [
            pltpu.make_async_copy(leg_hbm.at[s, pl.ds(k * size, size), :], leg.at[s, pl.ds(k * size, size), :], leg_sems.at[s, k])
            for s in range(2)
        ]
        for k in range(2 * PIECES)
    ]
    for pair in big[:FLIGHT]:
        for copy in pair:
            copy.start()
    for copy in small:
        copy.wait()
    row = lax.broadcasted_iota(jnp.int32, (n.cols, n.span), 0)
    target = (row // n.layers) % FIELDS == 2
    tables = [[], []]
    for s in range(2):
        masked, live = live_spec(n, spec_ref[s], wave_ref[s])
        sums = layer_sums(n, masked, share_ref)
        for part in range(2):
            total_ref[2 * s + part : 2 * s + part + 1, :] = sums[part * 16 + 12 : part * 16 + 13, :]
        high_ref[s] = jnp.where(target, pltpu.roll(sums, n.cols - n.layers, 0), 0.0)
        leg[s, n.lats : n.lats + 8, :] = jnp.where(live[:8], 1.0, 0.0).astype(bf16)
        leg[s, n.lats + 8 : n.lats + 16, :] = jnp.full((8, n.span), (1 - wave_ref[s] % 2).astype(f32)).astype(bf16)
        scaled = masked * jnp.where(wave_ref[s] == 0, 1.0, 2.0)
        none = jnp.zeros_like(scaled[:16])
        for hemi in range(2):
            rows = []
            for parity in range(2):
                mine = wave_ref[s] % 2 == parity
                for part in range(2):
                    chunk = jnp.where(mine, scaled[part * 16 : part * 16 + 16], 0.0)
                    rows += [chunk, none] if hemi == 0 else [none, chunk]
            tables[hemi].append(jnp.concatenate(rows, 0).astype(bf16))
    tables = [jnp.concatenate(pair, 1) for pair in tables]
    even = jnp.where(wave_ref[0] % 2 == 0, wave_ref[0], wave_ref[1])
    lane = lax.broadcasted_iota(jnp.int32, (8, LANES), 1)
    tag = jnp.where(lane < LANES // 2, even // 16, even % 16).astype(f32).astype(bf16)
    for owner in range(n.n_wave):
        out_ref[owner, n.rows : n.sent, :] = tag

    def strip(start, count):
        return out_ref.at[:, pl.ds(start, count), :], out_hbm.at[:, pl.ds(start, count), :]

    leaving = fetch(((total_ref, total_hbm), (high_ref, high_hbm), strip(n.rows, 8)), done_sems)
    for k in range(2 * PIECES):
        for copy in big[k]:
            copy.wait()
        if k + FLIGHT < 2 * PIECES:
            for copy in big[k + FLIGHT]:
                copy.start()
        rows = slice(k * size, (k + 1) * size)
        both = jnp.concatenate([leg[0, rows, :], leg[1, rows, :]], 1)
        acc[rows, :] = nt(both, tables[k // PIECES])
        if k >= PIECES and (k + 1) % (PIECES // 2) == 0:
            b = 3 - (k + 1) // (PIECES // 2) + 1
            for owner in range(n.n_wave):
                starts = n.block_starts(owner)
                block = acc[starts[0][b] : starts[0][b] + n.half, :] + acc[starts[1][b] : starts[1][b] + n.half, :]
                out_ref[owner, b * n.half : (b + 1) * n.half, :] = block.astype(bf16)
            copy = pltpu.make_async_copy(*strip(b * n.half, n.half), out_sems.at[b])
            copy.start()
            leaving.append(copy)
    for copy in leaving:
        copy.wait()


def grid_kernel(n, got_ref, sign_ref, near_ref, quad_hbm, total_hbm, out_hbm, pair_hbm, keep_hbm, spread, table_a, table_b, coef_a, coef_b, rows, out, total_ref, pair_ref, keep_ref, quad_ref, out_sems, in_sems, side_sems, inv_ref, cor_ref):
    arriving = fetch(((quad_hbm, quad_ref), (total_hbm, total_ref)), in_sems)
    device = lax.axis_index("wave")
    first_circle = device * n.half
    top = n.span - 1
    lane = lax.broadcasted_iota(jnp.int32, (8, LANES), 1)
    lane_f = lane.astype(f32)
    north = (lane // 4) % 2 == 0
    sent_lane = lax.broadcasted_iota(jnp.int32, (LANES, LANES), 0)
    to = lax.broadcasted_iota(jnp.int32, (LANES, LANES), 1)
    source = (to // 4 % 2) * 16 + (to // 8 % FIELDS) * 4 + to % 4
    for p in range(4):
        pick = jnp.where(sent_lane == source + p * 32, sign_ref[p : p + 1, :], 0.0).astype(bf16)
        wide = nn(got_ref[...], pick)
        for src in range(n.n_wave):
            for r in range(0, n.rows, 8):
                spread[p, pl.ds(r * n.n_wave + src, 8, stride=n.n_wave), :] = wide[src * n.sent + r : src * n.sent + r + 8]
    raw = got_rows_f32(n, got_ref)
    tag = jnp.where(lane < LANES // 2, raw * 16.0, raw)
    even_m = tag + pltpu.roll(tag, LANES // 2, 1)
    odd_m = float(top) - even_m
    even_2 = 2.0 * even_m
    odd_2 = 2.0 * odd_m
    for k in range(2):
        step = lax.broadcasted_iota(jnp.int32, (n.half, LANES), 0)
        circle = first_circle + step if k == 0 else n.circles - 1 - first_circle - step
        inv_ref[k] = 1.0 / (20 + 4 * circle).astype(f32)
        whole = jnp.full((n.half, LANES), 4.0 * n.lats, f32)
        cosine, _ = cos_sin((2 * circle + 1).astype(f32), whole, 1.0 / (4 * n.lats))
        cor_ref[k] = 2.0 * cosine
    tile_point = (lax.broadcasted_iota(jnp.int32, (8, LANES), 0) * LANES + lane).astype(f32)

    def sizes(i):
        short = first_circle + i
        return short, n.circles - 1 - short

    def build(i, u, table):
        short, long = sizes(i)
        cut = (short + 6).astype(f32)
        len_s = (20 + 4 * short).astype(f32)
        len_l = (20 + 4 * long).astype(f32)
        inv_s = inv_ref[0, pl.ds(i, 1), :]
        inv_l = inv_ref[1, pl.ds(i, 1), :]

        def places(point):
            own = point < cut
            return jnp.where(own, point, point - cut), jnp.where(own, len_s, len_l), jnp.where(own, inv_s, inv_l)

        j, length, inverse = places(tile_point)
        top_c, top_s = cos_sin(j * float(top), length, inverse)
        for t in range(n.tiles):
            j, length, inverse = places(lane_f + float(t * LANES))
            c, s = cos_sin(even_m * j, length, inverse)
            tc = jnp.broadcast_to(top_c[t : t + 1, :], (8, LANES))
            ts = jnp.broadcast_to(top_s[t : t + 1, :], (8, LANES))
            span = slice(t * LANES, (t + 1) * LANES)
            table[u, 0:8, span] = c
            table[u, 8:16, span] = s
            table[u, 16:24, span] = tc * c + ts * s
            table[u, 24:32, span] = ts * c - tc * s

    def gather(i, u, coef):
        short, long = sizes(i)
        parts = []
        for circle, row_n, row_s in (
            (short, i, n.half - 1 - i),
            (long, n.rows - 1 - i, n.half + i),
        ):
            length = (20 + 4 * circle).astype(f32)
            for p in range(4):
                up = spread[p, pl.ds(row_n * 8, 8), :]
                down = spread[p, pl.ds(row_s * 8, 8), :]
                seen = (odd_2 if p > 1 else even_2) < length
                parts.append(jnp.where(seen, jnp.where(north, up, down), 0.0))
        coef[u] = jnp.transpose(jnp.concatenate(parts, 0))

    south = lax.broadcasted_iota(jnp.int32, (8, LANES), 0) // 4
    lane_b = lax.broadcasted_iota(jnp.int32, (16, LANES), 1).astype(f32).astype(bf16)
    signs = [sign_ref[p : p + 1, :] for p in range(4)]
    group = lane // 32
    kinetic = jnp.where((lane // 8) % FIELDS == 2, 0.5, 1.0)

    def weights(t, cut):
        edge_at = jnp.clip(cut - t * LANES, -4, LANES + 4).astype(f32) - 0.5
        x = jnp.full((16, LANES), edge_at, f32).astype(bf16) - lane_b
        share = jnp.minimum(jnp.abs(x), 1.0)
        own = jnp.minimum(jnp.maximum(x + 0.5, 0.0), 1.0)
        if t == 0 or (t + 1) * LANES >= n.points:
            point = lax.broadcasted_iota(jnp.int32, (16, LANES), 1) + t * LANES
            ends = (point == 0) | (point == n.points - 1)
            share = share * jnp.where(ends, 0.5, jnp.where(point < n.points, 1.0, 0.0)).astype(bf16)
        own_share = own * share
        return own, 1.0 - own, own_share, share - own_share

    def transform(i, u, table, coef):
        short, long = sizes(i)
        cut = short + 6
        left = coef[u].astype(bf16)
        cor_s = cor_ref[0, pl.ds(i, 1), :]
        cor_l = cor_ref[1, pl.ds(i, 1), :]
        total = None
        for c in range(n.width // CHUNK):
            ahead, behind, spins = [], [], []
            for t in range(c * CHUNK // LANES, (c + 1) * CHUNK // LANES):
                tab = table[u, :, t * LANES : (t + 1) * LANES].astype(bf16)
                own, rest, own_share, rest_share = weights(t, cut)
                if c * CHUNK >= n.circles // 2 + 6:
                    ahead.append(jnp.concatenate([jnp.zeros_like(tab), tab], 0))
                    share = own_share + rest_share
                    behind.append(jnp.concatenate([tab[:16] * share, tab[16:] * share], 0))
                    spins.append(jnp.where(south == 0, cor_l, -cor_l))
                    continue
                ahead.append(jnp.concatenate([tab[:16] * own, tab[16:] * own, tab[:16] * rest, tab[16:] * rest], 0))
                behind.append(
                    jnp.concatenate(
                        [tab[:16] * own_share, tab[16:] * own_share, tab[:16] * rest_share, tab[16:] * rest_share], 0
                    )
                )
                spin = jnp.where(lane < cut - t * LANES, cor_s, cor_l)
                spins.append(jnp.where(south == 0, spin, -spin))
            grid = nn(left, jnp.concatenate(ahead, 1)).reshape(IMAGES, FIELDS, 8, CHUNK)
            x, y, curl, warm = grid[:, 0], grid[:, 1], grid[:, 2], grid[:, 3]
            absolute = curl + jnp.concatenate(spins, 1)
            prods = jnp.stack([absolute * x, absolute * y, x * x + y * y, x * warm], 1)
            piece = nt(jnp.concatenate(behind, 1), prods.reshape(LANES, CHUNK).astype(bf16))
            if piece.shape[0] < n.keys:
                piece = jnp.concatenate([jnp.zeros_like(piece), piece], 0)
            total = piece if total is None else total + piece
        results = []
        for k, circle in enumerate((short, long)):
            length = (20 + 4 * circle).astype(f32)
            folded = None
            for p in range(4):
                y = total[(4 * k + p) * 8 : (4 * k + p + 1) * 8] * signs[p]
                y = y + pltpu.roll(y, 64, 1)
                y = y + pltpu.roll(y, 32, 1)
                y = jnp.where((odd_2 if p > 1 else even_2) < length, y, 0.0)
                folded = y if folded is None else jnp.where(group == p, y, folded)
            weight = jnp.where(north, quad_ref[circle], quad_ref[n.lats - 1 - circle])
            results.append(folded * (weight * (inv_ref[k, pl.ds(i, 1), :] * kinetic)))
        return results

    turns = [i for k in range(n.half // 2) for i in (k, n.half - 1 - k)]
    groups = [turns[k : k + GROUP] for k in range(0, n.half, GROUP)]

    def ready(members, table, coef):
        for u, i in enumerate(members):
            build(i, u, table)
            gather(i, u, coef)

    def work(members, table, coef):
        for u in range(0, GROUP, 2):
            i, other = members[u : u + 2]
            short_i, long_i = transform(i, u, table, coef)
            short_o, long_o = transform(other, u + 1, table, coef)
            for at, up, down in (
                (i, short_i, short_o),
                (other, short_o, short_i),
                (n.half + i, long_o, long_i),
                (n.half + other, long_i, long_o),
            ):
                rows[pl.ds(at, 8, stride=n.rows), :] = jnp.where(north, up, down)

    ready(groups[0], table_a, coef_a)
    for copy in arriving:
        copy.wait()
    pair_ref[...] = total_ref[...] + near_ref[...]
    keep_ref[...] = jnp.where(lax.axis_index("lev") % 2 == 0, near_ref[...], 0.0)
    leaving = fetch(((pair_ref, pair_hbm), (keep_ref, keep_hbm)), side_sems)
    buffers = ((table_a, coef_a), (table_b, coef_b))
    sent_rows = 0
    for k, members in enumerate(groups):
        if k + 1 < len(groups):
            ready(groups[k + 1], *buffers[(k + 1) % 2])
        work(members, *buffers[k % 2])
        done = (k + 1) * GROUP // 2
        for r in range(sent_rows, n.half // 2 if done == n.half // 2 else done // 8 * 8, 8):
            sent_rows = r + 8
            for start in sorted({r, n.half - 8 - r, n.half + r, n.rows - 8 - r}):
                for src in range(n.n_wave):
                    at = src * n.rows + start
                    out[src, start : start + 8, :] = rows[at : at + 8, :].astype(bf16)
                copy = pltpu.make_async_copy(
                    out.at[:, pl.ds(start, 8), :], out_hbm.at[:, pl.ds(start, 8), :], out_sems.at[start // 8]
                )
                copy.start()
                leaving.append(copy)

    for copy in leaving:
        copy.wait()


def got_rows_f32(n, got_ref):
    pieces = [got_ref[src * n.sent + n.rows : src * n.sent + n.rows + 8, :].astype(f32)[:1] for src in range(n.n_wave)]
    return jnp.concatenate(pieces, 0)


def back_kernel(n, far_hbm, keep_hbm, high_hbm, back_ref, order_ref, leg, out_ref, turn, far_ref, keep_ref, high_ref, sems):
    arriving = fetch(((far_hbm, far_ref), (keep_hbm, keep_ref), (high_hbm, high_ref)), sems)
    for owner in range(n.n_wave):
        starts = n.block_starts(owner)
        for b in range(2):
            block = back_ref[owner * n.rows + b * n.half : owner * n.rows + (b + 1) * n.half, :]
            for hemi in range(2):
                at = starts[hemi][b] - hemi * n.circles
                turn[hemi, at : at + n.half, :] = block
    turned = [nt(order_ref[hemi * 64 : hemi * 64 + 64, :], turn[hemi]) for hemi in range(2)]
    row = lax.broadcasted_iota(jnp.int32, (n.cols, n.span), 0)
    target = (row // n.layers) % FIELDS == 2
    sums = []
    for s in range(2):
        even = leg[s, n.lats + 8 : n.lats + 16, :].astype(f32)[:1] > 0.5
        for hemi in range(2):
            mine = jnp.where(even, turned[hemi][:32], turned[hemi][32:]).astype(bf16)
            piece = nn(mine, leg[s, hemi * n.circles : (hemi + 1) * n.circles, :])
            sums.append(piece if hemi == 0 else sums.pop() + piece)
    for copy in arriving:
        copy.wait()
    deeper = keep_ref[...] + jnp.where(lax.axis_index("lev") < n.n_lev // 2, far_ref[...], 0.0)
    for s in range(2):
        live = leg[s, n.lats : n.lats + 8, :].astype(f32)[:1] > 0.5
        low = jnp.where(row < 16, deeper[2 * s : 2 * s + 1], deeper[2 * s + 1 : 2 * s + 2])
        tendency = sums[s] + high_ref[s] + jnp.where(target, low, 0.0)
        out_ref[s] = jnp.where(live, tendency, 0.0).astype(bf16)


def stay(*arrays, space=pltpu.HBM):
    return [pltpu.with_memory_space_constraint(x, space) for x in arrays]


def kernel_params():
    return pltpu.CompilerParams(
        vmem_limit_bytes=24 * 1024 * 1024
    )


def smem():
    return pl.BlockSpec(memory_space=pltpu.SMEM)


def vmem():
    return pl.BlockSpec(memory_space=pltpu.VMEM)


def hbm():
    return pl.BlockSpec(memory_space=pltpu.HBM)


def grid_call(n, got, quad_weight, totals, near):
    all_rows = n.n_wave * n.rows
    signs = np.zeros((8, LANES), np.float32)
    signs[:4] = np.repeat(image_signs(), LANES // IMAGES, axis=1)
    table = pltpu.VMEM((GROUP, n.keys // 2, n.width), f32)
    coef = pltpu.VMEM((GROUP, LANES, n.keys), f32)
    return pl.pallas_call(
        lambda *refs: grid_kernel(n, *refs),
        out_shape=(pltpu.HBM((n.n_wave, n.rows, LANES), bf16), pltpu.HBM(totals.shape, f32), pltpu.HBM(totals.shape, f32)),
        in_specs=[vmem()] * 3 + [hbm()] * 2,
        out_specs=(hbm(),) * 3,
        scratch_shapes=[
            pltpu.VMEM((4, n.n_wave * n.rows, LANES), f32),
            table,
            table,
            coef,
            coef,
            pltpu.VMEM((all_rows, LANES), f32),
            pltpu.VMEM((n.n_wave, n.rows, LANES), bf16),
            pltpu.VMEM(totals.shape, f32),
            pltpu.VMEM(totals.shape, f32),
            pltpu.VMEM(totals.shape, f32),
            pltpu.SMEM((n.lats,), f32),
            pltpu.SemaphoreType.DMA((n.rows // 8,)),
            pltpu.SemaphoreType.DMA((2,)),
            pltpu.SemaphoreType.DMA((2,)),
            pltpu.VMEM((2, n.half, LANES), f32),
            pltpu.VMEM((2, n.half, LANES), f32),
        ],
        compiler_params=kernel_params(),
        name="grid_stage",
    )(
        got,
        jnp.asarray(signs),
        near,
        *stay(quad_weight, totals),
    )


def fast_body(n, spec, legendre, layer_depth_share, quad_weight, wave_of_slot):
    params = kernel_params()
    all_rows = n.n_wave * n.rows
    dma = pltpu.SemaphoreType.DMA
    held_shape = (2, n.lats + 16, n.span)
    high_shape = (2, n.cols, n.span)
    total_shape = (4, n.span)
    sent, totals, held, high = pl.pallas_call(
        lambda *refs: forward_kernel(n, *refs),
        out_shape=(
            pltpu.HBM((n.n_wave, n.sent, LANES), bf16),
            pltpu.HBM(total_shape, f32),
            pltpu.VMEM(held_shape, bf16),
            pltpu.HBM(high_shape, f32),
        ),
        in_specs=[hbm()] * 4,
        out_specs=(hbm(), hbm(), vmem(), hbm()),
        scratch_shapes=[
            pltpu.SMEM((2,), jnp.int32),
            pltpu.SMEM((n.layers,), f32),
            pltpu.VMEM(spec.shape, bf16),
            pltpu.VMEM(total_shape, f32),
            pltpu.VMEM(high_shape, f32),
            pltpu.VMEM((n.lats, LANES), f32),
            dma((3,)),
            dma((2, 2 * PIECES)),
            dma((3,)),
            pltpu.VMEM((n.n_wave, n.sent, LANES), bf16),
            dma((2,)),
        ],
        compiler_params=params,
        name="legendre_forward",
    )(*stay(wave_of_slot, layer_depth_share, spec, legendre))
    near = lax.ppermute(totals, "lev", [(i, i ^ 1) for i in range(n.n_lev)])
    got = lax.all_to_all(sent, "wave", split_axis=0, concat_axis=0, tiled=True)
    out, pair, keep = grid_call(n, got.reshape(n.n_wave * n.sent, LANES), quad_weight, totals, near)
    far = lax.ppermute(pair, "lev", [(i, i ^ 2) for i in range(n.n_lev)])
    back = lax.all_to_all(
        out, "wave", split_axis=0, concat_axis=0, tiled=True
    )
    return pl.pallas_call(
        lambda *refs: back_kernel(n, *refs),
        out_shape=jax.ShapeDtypeStruct(spec.shape, bf16),
        in_specs=[hbm()] * 3 + [vmem()] * 3,
        out_specs=vmem(),
        scratch_shapes=[
            pltpu.VMEM((2, n.circles, LANES), bf16),
            pltpu.VMEM(total_shape, f32),
            pltpu.VMEM(total_shape, f32),
            pltpu.VMEM(high_shape, f32),
            dma((3,)),
        ],
        compiler_params=params,
        name="legendre_back",
    )(
        *stay(far, keep, high),
        back.reshape(all_rows, LANES),
        jnp.asarray(order_matrix(n), bf16),
        *stay(held, space=pltpu.VMEM),
    )


full_turn = 2.0 * math.pi


def carried_in(part, axis, combine, identity):
    count = lax.axis_size(axis)
    place = lax.axis_index(axis)
    ahead = count - 1 - place
    gathered = lax.all_gather(part, axis)
    state = jnp.zeros_like(part) + jnp.asarray(identity, part.dtype)

    def one(hop, state):
        source = count - 1 - hop
        return combine(state, lax.dynamic_index_in_dim(gathered, source, 0, False))

    return lax.fori_loop(0, ahead, one, state)


def rate_bundle(
    eastward_velocity,
    northward_velocity,
    local_curl_spin,
    thermal_state,
    planetary_rotation_effect,
    processor_dimension,
):
    absolute = local_curl_spin + planetary_rotation_effect
    return jnp.stack(
        [
            absolute * eastward_velocity,
            absolute * northward_velocity,
            0.5 * (eastward_velocity * eastward_velocity + northward_velocity * northward_velocity),
            eastward_velocity * thermal_state,
        ],
        axis=processor_dimension,
    )


def row_latitudes(device, per_dev, total_lat):
    row_ids = jnp.arange(per_dev, dtype=jnp.int32)
    quarter = per_dev // 4
    block_ids = row_ids // 4
    hemisphere = row_ids // 2 % 2
    member = row_ids % 2
    first_dist = device * quarter + block_ids
    pole_dist = jnp.where(member == 0, first_dist, total_lat // 2 - 1 - first_dist)
    return jnp.where(hemisphere == 0, pole_dist, total_lat - 1 - pole_dist)


def add_terms(earlier, later):
    return earlier + later


def general_body(spec, legendre, layer_depth_share, quad_weight, wave_of_slot):
    number_of_slots, columns, degree_list = spec.shape
    total_lat = legendre.shape[1]
    groups = lax.axis_size("wave")
    device = lax.axis_index("wave")
    per_dev = total_lat // groups
    layers_on_processor = layer_depth_share.shape[0]
    field_stack = columns // (2 * layers_on_processor)
    flat_rows = field_stack * layers_on_processor
    max_points = 20 + 4 * (total_lat // 2 - 1)
    all_waves = lax.all_gather(wave_of_slot, "wave", axis=0, tiled=True)
    wave_count = all_waves.shape[0]
    weight_two = jnp.where(all_waves == 0, 1.0, 2.0).astype(jnp.float32)
    degree_index = jnp.arange(degree_list, dtype=jnp.int32)
    valid_cols = degree_index[None, :] < (degree_list - wave_of_slot)[:, None]
    screened_entries = jnp.where(valid_cols[:, None, :], spec, jnp.zeros_like(spec))
    thermal_state = screened_entries.reshape(
        number_of_slots, 2, field_stack, layers_on_processor, degree_list
    )[:, :, 3].astype(jnp.float32)
    scaled_entries = thermal_state * layer_depth_share[None, None, :, None]
    below_sum = jnp.flip(jnp.cumsum(jnp.flip(scaled_entries, 2), 2), 2)
    deeper = carried_in(
        below_sum[:, :, 0],
        "lev",
        add_terms,
        jnp.zeros((number_of_slots, 2, degree_list), jnp.float32),
    )
    geopot = below_sum + deeper[:, :, None, :]
    fourier = jnp.einsum(
        "sln,scn->lsc", legendre, screened_entries, preferred_element_type=jnp.float32
    ).astype(jnp.bfloat16)
    send_order = row_latitudes(
        jnp.arange(groups, dtype=jnp.int32)[:, None], per_dev, total_lat
    ).reshape(-1)
    send_rows = jnp.take(fourier, send_order, axis=0).reshape(total_lat, number_of_slots * columns)
    received = lax.all_to_all(send_rows, "wave", split_axis=0, concat_axis=1, tiled=True)
    coeffs = received.reshape(per_dev, wave_count, 2, flat_rows)
    latitudes = row_latitudes(device, per_dev, total_lat)
    lengths = 20 + 4 * jnp.minimum(latitudes, total_lat - 1 - latitudes)
    planetary_rotation_effect = 2.0 * jnp.cos(
        (latitudes.astype(jnp.float32) + 0.5) * (math.pi / total_lat)
    )
    row_scale = quad_weight[latitudes] / lengths.astype(jnp.float32)
    quarter = per_dev // 4
    pair_points = max_points + 20
    tile_count = -(-pair_points // 128)
    padded = tile_count * 128
    pair_len = lengths.reshape(quarter, 2, 2)[:, 0, :]
    first_len = pair_len[:, 0:1]
    second_len = pair_len[:, 1:2]
    points = jnp.arange(padded, dtype=jnp.int32)[None, :]
    first_lat = points < first_len
    in_pair = points < pair_points
    local_idx = jnp.where(first_lat, points, points - first_len)
    point_len = jnp.where(first_lat, first_len, second_len)
    phase_int = all_waves[None, :, None] * local_idx[:, None, :] % point_len[:, None, :]
    angles = phase_int.astype(jnp.float32) * full_turn / point_len.astype(jnp.float32)[:, None, :]
    cosine = jnp.cos(angles)
    sine_vals = jnp.sin(angles)
    resolved = (2 * all_waves[None, :, None] < point_len[:, None, :]) & in_pair[:, None, :]
    amplitude = jnp.where(resolved, weight_two[None, :, None], 0.0)
    forward_tab = jnp.concatenate([amplitude * cosine, -(amplitude * sine_vals)], 1).astype(
        jnp.bfloat16
    )
    back_tab = jnp.concatenate(
        [jnp.where(resolved, cosine, 0.0), -jnp.where(resolved, sine_vals, 0.0)], 1
    ).astype(jnp.bfloat16)
    forward_tiles = forward_tab.reshape(quarter, 2 * wave_count, tile_count, 128)
    back_tiles = back_tab.reshape(quarter, 2 * wave_count, tile_count, 128)
    tile_start = jnp.arange(tile_count, dtype=jnp.int32)[None, :] * 128
    owner_second = tile_start + 128 > first_len
    boundary = first_len[:, 0] // 128
    is_bound = jnp.arange(tile_count, dtype=jnp.int32)[None, :] == boundary[:, None]
    first_tiles = first_lat.reshape(quarter, tile_count, 128)
    stacked = coeffs.reshape(quarter, 2, 2, wave_count, 2, flat_rows).transpose(0, 1, 2, 4, 3, 5)
    stacked = stacked.reshape(quarter, 2, 2, 2 * wave_count, flat_rows)
    coef_tiles = jnp.where(
        owner_second[:, None, :, None, None],
        stacked[:, :, 1][:, :, None],
        stacked[:, :, 0][:, :, None],
    )
    grid_tiles = jnp.einsum(
        "qatkf,qktp->qaftp", coef_tiles, forward_tiles, preferred_element_type=jnp.float32
    )
    bound_fwd = jnp.take_along_axis(forward_tiles, boundary[:, None, None, None], axis=2)[:, :, 0]
    bound_back = jnp.take_along_axis(back_tiles, boundary[:, None, None, None], axis=2)[:, :, 0]
    edge_grid = jnp.einsum(
        "qakf,qkp->qafp", stacked[:, :, 0], bound_fwd, preferred_element_type=jnp.float32
    )
    use_edge = is_bound[:, :, None] & first_tiles
    grid_tiles = jnp.where(use_edge[:, None, None], edge_grid[:, :, :, None, :], grid_tiles)
    grid_vals = grid_tiles.reshape(quarter, 2, field_stack, layers_on_processor, padded)
    row_cor = planetary_rotation_effect.reshape(quarter, 2, 2)
    point_cor = jnp.where(first_lat[:, None, :], row_cor[:, :, 0:1], row_cor[:, :, 1:2])[
        :, :, None, :
    ]
    products = rate_bundle(
        grid_vals[:, :, 0], grid_vals[:, :, 1], grid_vals[:, :, 2], grid_vals[:, :, 3], point_cor, 2
    )
    products = products.astype(jnp.bfloat16).reshape(quarter, 2, flat_rows, tile_count, 128)
    keep = jnp.where(owner_second[:, :, None], jnp.logical_not(first_tiles), first_tiles)
    main_prods = jnp.where(keep[:, None, None], products, jnp.zeros_like(products))
    per_tile = jnp.einsum(
        "qaftp,qktp->qatkf", main_prods, back_tiles, preferred_element_type=jnp.float32
    )
    bound_prods = jnp.take_along_axis(products, boundary[:, None, None, None, None], axis=3)[
        :, :, :, 0
    ]
    bound_first = jnp.take_along_axis(first_tiles, boundary[:, None, None], axis=1)[:, 0]
    bound_prods = jnp.where(bound_first[:, None, None, :], bound_prods, jnp.zeros_like(bound_prods))
    edge_back = jnp.einsum(
        "qafp,qkp->qakf", bound_prods, bound_back, preferred_element_type=jnp.float32
    )
    owner_mask = owner_second[:, None, :, None, None]
    first_ret = jnp.sum(jnp.where(owner_mask, 0.0, per_tile), axis=2) + edge_back
    second_ret = jnp.sum(jnp.where(owner_mask, per_tile, 0.0), axis=2)
    returned = jnp.stack([first_ret, second_ret], axis=2)
    returned = (returned * row_scale.reshape(quarter, 2, 2)[:, :, :, None, None]).astype(
        jnp.bfloat16
    )
    out_rows = returned.reshape(quarter, 2, 2, 2, wave_count, flat_rows).transpose(0, 1, 2, 4, 3, 5)
    out_rows = out_rows.reshape(per_dev, wave_count * columns)
    gathered_rows = lax.all_to_all(out_rows, "wave", split_axis=1, concat_axis=0, tiled=True)
    inverse = (
        jnp.zeros((total_lat,), jnp.int32)
        .at[send_order]
        .set(jnp.arange(total_lat, dtype=jnp.int32))
    )
    back_fourier = jnp.take(gathered_rows, inverse, axis=0).reshape(
        total_lat, number_of_slots, columns
    )
    tendency = jnp.einsum(
        "lsc,sln->scn", back_fourier, legendre, preferred_element_type=jnp.float32
    )
    tendency = tendency.reshape(number_of_slots, 2, field_stack, layers_on_processor, degree_list)
    tendency = tendency.at[:, :, 2].add(geopot)
    tendency = jnp.where(valid_cols[:, None, None, None, :], tendency, 0.0)
    return tendency.reshape(number_of_slots, columns, degree_list).astype(jnp.bfloat16)


def solution(mesh):
    def body(spec, legendre, layer_depth_share, quad_weight, wave_of_slot):
        slots, cols, span = spec.shape
        layers = layer_depth_share.shape[0]
        n = Sizes(mesh.shape["wave"], mesh.shape["lev"], slots, cols, legendre.shape[1], span, layers)
        step = (lambda *args: fast_body(n, *args)) if n.fits() else general_body
        return step(spec, legendre, layer_depth_share, quad_weight, wave_of_slot)

    in_specs = (P("wave", "lev", None), P("wave", None, None), P("lev"), P(), P("wave"))
    out_specs = P("wave", "lev", None)
    return jax.shard_map(body, mesh=mesh, in_specs=in_specs, out_specs=out_specs, check_vma=False)
```
